32 devices in a mesh: tm: 4 (over y, x), orig: 8 (over z, core).
Axes of the slice: x: 2, y: 2, z: 4, core: 2. Of those that a mesh axis runs over, the one named last changes fastest.
Arguments:
- trip_counts: bfloat16 [12, 96, 256, 256], P('tm', 'orig'), may hold values from 0.25 to 4
- anchor_hour: float32 [12, 2048], P('tm', 'orig'), may hold values from 100 to 3000
- dest_hour: float32 [12, 32768], P('tm'), may hold values from 100 to 3000
- daily_target: bfloat16 [96, 256, 256], P('orig'), may hold values from 2 to 40
- block_columns: int32 [96], P('orig'), may hold values from -1 to 127, as said below
Outputs:
- fitted: bfloat16 [12, 96, 256, 256], P('tm', 'orig')
- dest_gap: float32 [12, 32768], P('tm', 'orig')
The draws below stay inside these ranges and needn't reach their ends.
Inputs may be any that keep to these rules, and one draw needn't show every extreme that they name: `block_columns`: within each anchor block row the live column numbers are distinct and come first, followed by -1 for empty slots; every block row has at least one live slot, and some block row has all 12 live.
All inputs are finite; a program needn't handle non-finite values.
Results may differ from the reference program's by a relative error of at most 0.001.
Values sent between devices are 32-bit elements; how exact they have to be, the bound alone decides.
No kernel may reach another device: no remote copies, remote signals or barrier semaphores. Data moves between devices by JAX's collectives and lax.ppermute only.
A program may use at most 64 MiB of HBM per device.

```python
import math
import jax
import jax.numpy as jnp
from jax import lax

BLOCK = 256
ZONES = 32768
SLOTS = 12
BINS = 12
COLS = 128
ANCHORS = 2048
SLOTS_ALL = 96
N_ORIG = 8


def draw_block_columns(key, part):
    devices = SLOTS_ALL // SLOTS
    key_list = jax.random.split(key, 4)

    def one_order(row_key):
        return jax.random.permutation(row_key, COLS)
    orders = jax.vmap(one_order)(jax.random.split(key_list[0], devices))[:, :SLOTS]
    small_count = 1 + jax.random.randint(key_list[1], (devices,), 0, max(SLOTS // 2, 1))
    full_draw = jax.random.randint(key_list[2], (devices,), 0, 8)
    chosen_device = jax.random.randint(key_list[3], (), 0, devices)
    counts = jnp.where((full_draw == 0) | (jnp.arange(devices) == chosen_device), SLOTS, small_count)
    slot_index = jnp.arange(SLOTS)[None, :]
    return jnp.where(slot_index < counts[:, None], orders, -1).astype(jnp.int32).reshape(-1)


def levels(key, extent, cuts, smallest, largest):
    def one(dim, shards_of):
        heights = jax.random.uniform(jax.random.fold_in(jax.random.fold_in(key, 6), dim), (shards_of,), jnp.float32, smallest / len(cuts), largest / len(cuts))
        return jnp.repeat(jnp.exp(heights), extent[dim] // shards_of).reshape((-1,) + (1,) * (len(extent) - dim - 1))

    level = one(*cuts[0])
    for cut in cuts[1:]:
        level = level * one(*cut)
    return level


def setup_inputs(seed: int = 0) -> dict:
    streams_of = jax.random.split(jax.random.key(seed), 6)
    trip_counts = jnp.clip(jnp.exp(math.log(4.0) - 2.7725887 * jax.random.uniform(streams_of[0], (BINS, SLOTS_ALL, BLOCK, BLOCK), jnp.float32) ** levels(streams_of[0], (BINS, SLOTS_ALL, BLOCK, BLOCK), ((0, 4), (1, 8)), -0.2, 0.2)), 0.25, 4.0).astype(jnp.bfloat16)
    anchor_hour = jnp.clip(jnp.exp(math.log(3000.0) - 3.4011974 * jax.random.uniform(streams_of[1], (BINS, ANCHORS), jnp.float32) ** levels(streams_of[1], (BINS, ANCHORS), ((0, 4), (1, 8)), -0.2, 0.2)), 100.0, 3000.0)
    dest_hour = jnp.clip(jnp.exp(math.log(3000.0) - 3.4011974 * jax.random.uniform(streams_of[2], (BINS, ZONES), jnp.float32) ** levels(streams_of[2], (BINS, ZONES), ((0, 4),), -0.2, 0.2)), 100.0, 3000.0)
    daily_target = jnp.clip(jnp.exp(math.log(40.0) - 2.9957323 * jax.random.uniform(streams_of[3], (SLOTS_ALL, BLOCK, BLOCK), jnp.float32) ** levels(streams_of[3], (SLOTS_ALL, BLOCK, BLOCK), ((0, 8),), -0.2, 0.2)), 2.0, 40.0).astype(jnp.bfloat16)
    block_columns = draw_block_columns(jax.random.fold_in(streams_of[5], 71), 0)
    return dict(trip_counts=trip_counts, anchor_hour=anchor_hour, dest_hour=dest_hour, daily_target=daily_target, block_columns=block_columns)


def anchor_scaled(trip_block, anchor_block, live_mask):
    values = trip_block.astype(jnp.float32) * live_mask[None, :, None, None]
    row_sums = jnp.sum(values, axis=(1, 3))
    return values * (anchor_block / row_sums)[:, None, :, None]


def column_sums(values, onehot):
    return jnp.einsum("tsj,sc->tcj", jnp.sum(values, axis=2), onehot, precision=lax.Precision.HIGHEST)


def reference(trip_counts, anchor_hour, dest_hour, daily_target, block_columns):
    shaped = trip_counts.reshape(BINS, N_ORIG, SLOTS, BLOCK, BLOCK)
    columns = block_columns.reshape(N_ORIG, SLOTS)
    anchors = anchor_hour.reshape(BINS, N_ORIG, BLOCK)
    targets = daily_target.reshape(N_ORIG, SLOTS, BLOCK, BLOCK)

    def pieces(index):
        column_row = lax.dynamic_index_in_dim(columns, index, 0, keepdims=False)
        live_mask = (column_row >= 0).astype(jnp.float32)
        onehot = (column_row[:, None] == jnp.arange(COLS, dtype=jnp.int32)[None, :]).astype(jnp.float32)
        trip_block = lax.dynamic_index_in_dim(shaped, index, 1, keepdims=False)
        anchor_block = lax.dynamic_index_in_dim(anchors, index, 1, keepdims=False)
        return anchor_scaled(trip_block, anchor_block, live_mask), live_mask, onehot

    def first_pass(index, totals):
        anchor_fit, live_mask, onehot = pieces(index)
        return totals + column_sums(anchor_fit, onehot)

    zeros = jnp.zeros((BINS, COLS, BLOCK), jnp.float32)
    totals = lax.fori_loop(0, N_ORIG, first_pass, zeros)
    dest_gain = dest_hour.reshape(BINS, COLS, BLOCK) / jnp.maximum(totals, 1.0)

    def second_pass(index, state):
        fitted, after = state
        anchor_fit, live_mask, onehot = pieces(index)
        spread = jnp.einsum("sc,tcj->tsj", onehot, dest_gain, precision=lax.Precision.HIGHEST)
        dest_fit = anchor_fit * spread[:, :, None, :]
        daily_sum = jnp.sum(dest_fit, axis=0)
        target_block = lax.dynamic_index_in_dim(targets, index, 0, keepdims=False).astype(jnp.float32)
        daily_fit = dest_fit * (target_block / (daily_sum + 1.0 - live_mask[:, None, None]))[None]
        fitted = lax.dynamic_update_index_in_dim(fitted, daily_fit.astype(jnp.bfloat16), index, 1)
        return fitted, after + column_sums(daily_fit, onehot)

    fitted, after = lax.fori_loop(0, N_ORIG, second_pass, (jnp.zeros_like(shaped), zeros))
    dest_gap = after.reshape(BINS, ZONES) / dest_hour - 1.0
    return fitted.reshape(BINS, SLOTS_ALL, BLOCK, BLOCK), dest_gap
```

```python
import functools

import jax
import jax.numpy as jnp
from jax import lax
from jax.experimental import pallas as pl
from jax.experimental.pallas import tpu as pltpu
from jax.sharding import PartitionSpec as P


LANES = 128
F32 = jnp.float32


def whole(memory_space=pltpu.VMEM):
    return pl.BlockSpec(memory_space=memory_space)


def anchor_kernel(cols, anchor, trips, acol, sums):
    _, slots, side, _ = trips.shape
    halves = side // LANES
    bin_ = pl.program_id(0)
    count = pl.num_programs(0) * halves * slots

    @pl.when(bin_ == 0)
    def _():
        sums[...] = jnp.zeros(sums.shape, F32)
        for s in range(slots):
            sums[count + s : count + s + 1, :] = jnp.full((1, LANES), cols[s], jnp.int32).astype(F32)

    live = functools.reduce(lambda a, b: a + b, [(cols[s] >= 0).astype(jnp.int32) for s in range(slots)])
    rows = side // 4
    target = anchor[pl.ds(bin_, 1), :]
    for r in range(0, side, rows):

        def add(s, acc):
            return acc + trips[0, s, r : r + rows, :].astype(F32)

        total = jnp.sum(lax.fori_loop(0, live, add, jnp.zeros((rows, side), F32)), axis=1, keepdims=True)
        diagonal = (
            lax.broadcasted_iota(jnp.int32, (rows, side), 0) + r == lax.broadcasted_iota(jnp.int32, (rows, side), 1)
        )
        column = jnp.sum(jnp.where(diagonal, target, 0.0), axis=1, keepdims=True)
        acol[0, r : r + rows, :] = jnp.broadcast_to(column / total, (rows, LANES))

    def slot(s, _):
        for h in range(halves):
            scaled = trips[0, s, :, h * LANES : (h + 1) * LANES].astype(F32) * acol[0]
            row = (bin_ * halves + h) * slots + s
            sums[pl.ds(row, 1), :] = jnp.sum(scaled, axis=0, keepdims=True)
        return 0

    lax.fori_loop(0, live, slot, 0)


def lookup_kernel(where, cols, dest, picked, span):
    parts, slots, _ = picked.shape
    bins = dest.shape[0]
    halves = parts // bins
    side = halves * LANES
    for s in range(slots):
        start = pl.multiple_of(jnp.maximum(cols[s], 0) * side, side)
        row = dest[:, pl.ds(start, side)]
        for t in range(bins):
            for h in range(halves):
                picked[t * halves + h, s : s + 1, :] = row[t : t + 1, h * LANES : (h + 1) * LANES]
    width = span.shape[1]
    span[...] = dest[:, pl.ds(pl.multiple_of(where[0] * width, width), width)]


def matched(own, columns, values, parts, slots, first):
    acc = [jnp.zeros(own.shape, F32) for _ in range(parts)]
    for cref, vref in zip(columns, values):
        for k in range(cref.shape[0]):
            for s in range(slots):
                hit = own == cref[k, first + s : first + s + 1, :]
                for q in range(parts):
                    acc[q] = acc[q] + jnp.where(hit, vref[k, q * slots + s : q * slots + s + 1, :], 0.0)
    return acc


def gain_kernel(picked, *refs):
    parts, slots, _ = picked.shape
    arrived, gain = refs[:-1], refs[-1]
    first = parts * slots
    own = arrived[0][0, first : first + slots, :]
    total = matched(own, arrived, arrived, parts, slots, first)
    for q in range(parts):
        gain[q] = jnp.where(own >= 0.0, picked[q] / jnp.maximum(total[q], 1.0), 0.0)


def gap_kernel(where, span, *refs):
    out = refs[-1]
    n = (len(refs) - 1) // 2
    columns, values = refs[:n], refs[n : 2 * n]
    slots = columns[0].shape[1] - values[0].shape[1]
    first = values[0].shape[1]
    parts = first // slots
    bins = out.shape[0]
    halves = parts // bins
    side = halves * LANES
    blocks = out.shape[1] // side
    own = (lax.broadcasted_iota(jnp.int32, (blocks, LANES), 0) + where[0] * blocks).astype(F32)
    total = matched(own, columns, values, parts, slots, first)
    for t in range(bins):
        for h in range(halves):
            for c in range(blocks):
                at = c * side + h * LANES
                out[t : t + 1, at : at + LANES] = total[t * halves + h][c : c + 1, :]
    out[...] = out[...] / span[...] - 1.0


def day_part(trips, acol, gain, slot, h, bins, halves):
    acc = None
    for t in range(bins):
        g = gain[t * halves + h, pl.ds(slot, 1), :]
        part = trips[t, 0, :, h * LANES : (h + 1) * LANES].astype(F32) * acol[t] * g
        acc = part if acc is None else acc + part
    return acc


def send_kernel(bits, first_trips, second_trips, first_acol, second_acol, gain, first, second, *, start):
    bins = first_trips.shape[0]
    halves = first_trips.shape[3] // LANES
    slot = pl.program_id(0) + start
    for out, trips, acol in ((first, first_trips, first_acol), (second, second_trips, second_acol)):
        for h in range(halves):
            out[0, :, h * LANES : (h + 1) * LANES] = day_part(trips, acol, gain, slot, h, bins, halves)


def keep_kernel(
    bits, first_trips, second_trips, first_acol, second_acol, gain, first_in, second_in, first, second, *, start
):
    bins = first_trips.shape[0]
    halves = first_trips.shape[3] // LANES
    slot = pl.program_id(0) + start
    for out, got, trips, acol in (
        (first, first_in, first_trips, first_acol),
        (second, second_in, second_trips, second_acol),
    ):
        for h in range(halves):
            lanes = slice(h * LANES, (h + 1) * LANES)
            out[0, :, lanes] = day_part(trips, acol, gain, slot, h, bins, halves) + got[0, :, lanes]


def factor_kernel(bits, cols, ua, va, ub, vb, ta, tb, fa, fb, *, start):
    live = (cols[pl.program_id(0) + start] >= 0).astype(F32)
    fa[...] = ta[...].astype(F32) / (ua[...] + va[...] + 1.0 - live)
    fb[...] = tb[...].astype(F32) / (ub[...] + vb[...] + 1.0 - live)


def fit_kernel(bits, trips, acol, gain, fa, ga, fb, gb, sums_in, *refs, start, count, slots):
    fitted, sums = refs[-2], refs[-1]
    bins, _, side, _ = trips.shape
    halves = side // LANES
    rows = side // 4
    step = pl.program_id(0)
    slot = step + start

    @pl.when(step == 0)
    def _():
        sums[...] = sums_in[...]

    @pl.when(step < count)
    def _():
        places = (
            (bits[0], fa),
            (1 - bits[0], ga),
            (2 + bits[1], fb),
            (3 - bits[1], gb),
        )
        for t in range(bins):
            for h in range(halves):
                lanes = slice(h * LANES, (h + 1) * LANES)
                q = t * halves + h
                g = gain[q, pl.ds(slot, 1), :]
                total = jnp.zeros((1, LANES), F32)
                for block, factor in places:
                    at = pl.ds(pl.multiple_of(block * rows, rows), rows)
                    value = trips[t, 0, at, lanes].astype(F32) * acol[t, at, :] * g * factor[0, :, lanes]
                    fitted[t, 0, at, lanes] = value.astype(fitted.dtype)
                    total = total + jnp.sum(value, axis=0, keepdims=True)
                sums[pl.ds(q * slots + slot, 1), :] = total

    @pl.when(step >= count)
    def _():
        fitted[...] = jnp.zeros(fitted.shape, fitted.dtype)


def chunked(count, size):
    return [(start, min(size, count - start)) for start in range(0, count, size)]


def cycle(trips, acol, gain, target, cols, bits, *, count, size):
    bins, slots, side, _ = trips.shape
    halves = side // LANES
    rows = side // 4
    parts = bins * halves

    def over_first(x):
        return lax.ppermute(x, "tm", [(i, i ^ 2) for i in range(4)])

    def over_second(x):
        return lax.ppermute(x, "tm", [(i, i ^ 1) for i in range(4)])

    def call(kernel, start, size, keep, extra_specs, outs, extra):
        def block(first, b):
            bit = b[0] if first else b[1]
            return (0 if first else 2) + (bit if keep else 1 - bit)

        def trip_spec(first):
            return pl.BlockSpec((bins, 1, rows, side), lambda i, b: (0, start + i, block(first, b), 0))

        def acol_spec(first):
            return pl.BlockSpec((bins, rows, LANES), lambda i, b: (0, block(first, b), 0))

        part = pl.BlockSpec((1, rows, side), lambda i, b: (i, 0, 0))
        shape = jax.ShapeDtypeStruct((size, rows, side), F32)
        return pl.pallas_call(
            functools.partial(kernel, start=start),
            grid_spec=pltpu.PrefetchScalarGridSpec(
                num_scalar_prefetch=1,
                grid=(size,),
                in_specs=[trip_spec(True), trip_spec(False), acol_spec(True), acol_spec(False), whole()]
                + [part] * len(extra),
                out_specs=[part, part],
            ),
            out_shape=[shape, shape],
        )(bits, trips, trips, acol, acol, gain, *extra)

    def factors(start, size, ua, va, ub, vb):
        part = pl.BlockSpec((1, rows, side), lambda i, b: (i, 0, 0))
        shape = jax.ShapeDtypeStruct((size, rows, side), F32)
        return pl.pallas_call(
            functools.partial(factor_kernel, start=start),
            grid_spec=pltpu.PrefetchScalarGridSpec(
                num_scalar_prefetch=1,
                grid=(size,),
                in_specs=[whole(pltpu.SMEM)]
                + [part] * 4
                + [
                    pl.BlockSpec((1, rows, side), lambda i, b: (start + i, b[0], 0)),
                    pl.BlockSpec((1, rows, side), lambda i, b: (start + i, 2 + b[1], 0)),
                ],
                out_specs=[part, part],
            ),
            out_shape=[shape, shape],
        )(bits, cols, ua, va, ub, vb, target, target)

    def fit(start, size, fa, ga, fb, gb, sums, fitted, steps):
        part = pl.BlockSpec((1, rows, side), lambda i, b: (jnp.minimum(i, size - 1), 0, 0))
        slab = pl.BlockSpec((bins, 1, side, side), lambda i, b: (0, start + i, 0, 0))
        source = pl.BlockSpec((bins, 1, side, side), lambda i, b: (0, start + jnp.minimum(i, size - 1), 0, 0))
        before = [] if fitted is None else [fitted]
        return pl.pallas_call(
            functools.partial(fit_kernel, start=start, count=size, slots=slots),
            grid_spec=pltpu.PrefetchScalarGridSpec(
                num_scalar_prefetch=1,
                grid=(steps,),
                in_specs=[source, whole(), whole(), part, part, part, part, whole()]
                + [pl.BlockSpec(memory_space=pl.ANY)] * len(before),
                out_specs=[slab, whole()],
            ),
            out_shape=[
                jax.ShapeDtypeStruct(trips.shape, trips.dtype),
                jax.ShapeDtypeStruct((parts * slots, LANES), F32),
            ],
            input_output_aliases={9: 0} if before else {},
        )(bits, trips, acol, gain, fa, ga, fb, gb, sums, *before)

    chunks = chunked(count, size)
    sent = [call(send_kernel, s, n, False, [], None, ()) for s, n in chunks]
    got = [(over_first(a), over_second(b)) for a, b in sent]
    kept = [call(keep_kernel, s, n, True, [], None, g) for (s, n), g in zip(chunks, got)]
    other = [(over_second(a), over_first(b)) for a, b in kept]
    scale = [factors(s, n, k[0], o[0], k[1], o[1]) for (s, n), k, o in zip(chunks, kept, other)]
    back = [(over_first(a), over_second(b)) for a, b in scale]
    fitted = None
    sums = jnp.zeros((parts * slots, LANES), F32)
    for i, ((s, n), f, b) in enumerate(zip(chunks, scale, back)):
        steps = slots - s if i == len(chunks) - 1 else n
        fitted, sums = fit(s, n, f[0], b[0], f[1], b[1], sums, fitted, steps)
    return fitted, sums


def gather(x, n):
    def swap(y, k):
        return lax.ppermute(y, "orig", [(i, i ^ k) for i in range(n)])

    near = jnp.stack([x] + [swap(x, k) for k in range(n - 2, 0, -2)])
    return [near, swap(near, 1)]


def make(mesh):
    n_orig = mesh.shape["orig"]
    n_tm = mesh.shape["tm"]
    assert n_tm == 4 and n_orig & (n_orig - 1) == 0 and n_orig > 1

    def on_device(trip_counts, anchor_hour, dest_hour, daily_target, block_columns):
        bins, slots, side, _ = trip_counts.shape
        halves = side // LANES
        parts = bins * halves
        width = dest_hour.shape[1] // n_orig
        where = lax.axis_index("orig").astype(jnp.int32).reshape(1)
        tm = lax.axis_index("tm").astype(jnp.int32)
        bits = jnp.stack([tm // 2, tm % 2])

        acol, sums = pl.pallas_call(
            anchor_kernel,
            grid=(bins,),
            in_specs=[
                whole(pltpu.SMEM),
                whole(),
                pl.BlockSpec((1, slots, side, side), lambda t: (t, 0, 0, 0)),
            ],
            out_specs=[pl.BlockSpec((1, side, LANES), lambda t: (t, 0, 0)), whole()],
            out_shape=[
                jax.ShapeDtypeStruct((bins, side, LANES), F32),
                jax.ShapeDtypeStruct(((parts + 1) * slots, LANES), F32),
            ],
        )(block_columns, anchor_hour, trip_counts)
        arrived = gather(sums, n_orig)

        picked, span = pl.pallas_call(
            lookup_kernel,
            in_specs=[whole(pltpu.SMEM), whole(pltpu.SMEM), whole()],
            out_specs=[whole(), whole()],
            out_shape=[
                jax.ShapeDtypeStruct((parts, slots, LANES), F32),
                jax.ShapeDtypeStruct((bins, width), F32),
            ],
        )(where, block_columns, dest_hour)

        gain = pl.pallas_call(
            gain_kernel,
            in_specs=[whole()] * (1 + len(arrived)),
            out_specs=whole(),
            out_shape=jax.ShapeDtypeStruct((parts, slots, LANES), F32),
        )(picked, *arrived)

        live = jnp.sum((block_columns >= 0).astype(jnp.int32))
        counts = sorted({max(slots // 4, 1), max(slots // 2, 1), slots})
        pick = sum((live > c).astype(jnp.int32) for c in counts[:-1])
        fitted, final = lax.switch(
            pick,
            [functools.partial(cycle, count=c, size=3) for c in counts],
            trip_counts,
            acol,
            gain,
            daily_target,
            block_columns,
            bits,
        )
        finals = gather(final, n_orig)
        gap = pl.pallas_call(
            gap_kernel,
            in_specs=[whole(pltpu.SMEM), whole()] + [whole()] * (len(arrived) + len(finals)),
            out_specs=whole(),
            out_shape=jax.ShapeDtypeStruct((bins, width), F32),
        )(where, span, *arrived, *finals)
        return fitted, gap

    return on_device


def solution(mesh):
    placed = (
        P("tm", "orig", None, None),
        P("tm", "orig"),
        P("tm", None),
        P("orig", None, None),
        P("orig"),
    )
    return jax.shard_map(
        make(mesh),
        mesh=mesh,
        in_specs=placed,
        out_specs=(P("tm", "orig", None, None), P("tm", "orig")),
        check_vma=False,
    )
```

```python
import functools

import jax
import jax.numpy as jnp
from jax import lax
from jax.experimental import pallas as pl
from jax.experimental.pallas import tpu as pltpu
from jax.sharding import PartitionSpec as P


LANES = 128
F32 = jnp.float32
LIMIT = pltpu.CompilerParams(vmem_limit_bytes=8 * 2**20)


def whole(memory_space=pltpu.VMEM):
    return pl.BlockSpec(memory_space=memory_space)


def near(*xs):
    return [pltpu.with_memory_space_constraint(x, pltpu.VMEM) for x in xs]


def anchor_kernel(place, cols, anchor, trips, local, acol, sums, arrivals):
    bins, slots, side, _ = trips.shape
    halves = side // LANES
    rows = side // 4
    copies = [pltpu.make_async_copy(trips.at[t], local.at[t], arrivals.at[t]) for t in range(bins)]
    for copy in copies:
        copy.start()
    count = bins * halves * slots
    for s in range(slots):
        sums[count + s : count + s + 1, :] = jnp.full((1, LANES), cols[s], jnp.int32).astype(F32)
    live = [(cols[s] >= 0).astype(F32) for s in range(slots)]
    for t in range(bins):
        copies[t].wait()
        target = anchor[t : t + 1, :]
        acc = [[None] * halves for _ in range(slots)]
        for r in range(0, side, rows):
            total = None
            for s in range(slots):
                part = local[t, s, r : r + rows, :].astype(F32) * live[s]
                total = part if total is None else total + part
            total = jnp.sum(total, axis=1, keepdims=True)
            diagonal = (
                lax.broadcasted_iota(jnp.int32, (rows, side), 0) + r
                == lax.broadcasted_iota(jnp.int32, (rows, side), 1)
            )
            column = jnp.sum(jnp.where(diagonal, target, 0.0), axis=1, keepdims=True)
            scale = jnp.broadcast_to(column / total, (rows, LANES))
            acol[t, r : r + rows, :] = scale
            for s in range(slots):
                for h in range(halves):
                    part = local[t, s, r : r + rows, h * LANES : (h + 1) * LANES].astype(F32) * scale
                    part = jnp.sum(part.reshape(rows // 8, 8, LANES), axis=0)
                    acc[s][h] = part if acc[s][h] is None else acc[s][h] + part
        for h in range(halves):
            for s in range(slots):
                row = (t * halves + h) * slots + s
                sums[row : row + 1, :] = jnp.sum(acc[s][h], axis=0, keepdims=True)


def lookup_kernel(place, cols, dest, picked, span):
    parts, slots, _ = picked.shape
    bins = dest.shape[0]
    halves = parts // bins
    side = halves * LANES
    for s in range(slots):
        start = pl.multiple_of(jnp.maximum(cols[s], 0) * side, side)
        row = dest[:, pl.ds(start, side)]
        for t in range(bins):
            for h in range(halves):
                picked[t * halves + h, s : s + 1, :] = row[t : t + 1, h * LANES : (h + 1) * LANES]
    width = span.shape[1]
    span[...] = dest[:, pl.ds(pl.multiple_of(place[1] * width, width), width)]


def matched(own, columns, values, parts, slots, first):
    acc = [jnp.zeros(own.shape, F32) for _ in range(parts)]
    at = 0
    for vref in values:
        for k in range(vref.shape[0]):
            cref, c = (vref, k) if columns is None else (columns, at)
            at += 1
            for s in range(slots):
                hit = own == cref[c, first + s : first + s + 1, :]
                for q in range(parts):
                    acc[q] = acc[q] + jnp.where(hit, vref[k, q * slots + s : q * slots + s + 1, :], 0.0)
    return acc


def gain_kernel(picked, *refs):
    parts, slots, _ = picked.shape
    arrived, gain, columns = refs[:-2], refs[-2], refs[-1]
    first = parts * slots
    own = arrived[0][0, first : first + slots, :]
    total = matched(own, None, arrived, parts, slots, first)
    for q in range(parts):
        gain[q] = jnp.where(own >= 0.0, picked[q] / jnp.maximum(total[q], 1.0), 0.0)
    at = 0
    for ref in arrived:
        for k in range(ref.shape[0]):
            columns[at] = ref[k, first : first + slots, :]
            at += 1


def gap_kernel(place, span, *refs):
    out = refs[-1]
    columns, values = refs[0], refs[1:-1]
    slots = columns.shape[1]
    first = values[0].shape[1]
    parts = first // slots
    bins = out.shape[0]
    halves = parts // bins
    side = halves * LANES
    blocks = out.shape[1] // side
    own = (lax.broadcasted_iota(jnp.int32, (blocks, LANES), 0) + place[1] * blocks).astype(F32)
    total = matched(own, columns, values, parts, slots, 0)
    for t in range(bins):
        for h in range(halves):
            for c in range(blocks):
                at = c * side + h * LANES
                out[t : t + 1, at : at + LANES] = total[t * halves + h][c : c + 1, :]
    out[...] = out[...] / span[...] - 1.0


def blocks_of(place, kept):
    first, second = place[0] >> 1, place[0] & 1
    if kept:
        return first, 2 + second
    return 1 - first, 3 - second


def rows_of(block, rows):
    return pl.ds(pl.multiple_of(block * rows, rows), rows)


def day_kernel(place, cols, trips, acol, gain, *refs, ranges):
    bins, _, side, _ = trips.shape
    halves = side // LANES
    rows = side // 4
    outs, pick = refs[:-1], refs[-1]
    pick[0] = functools.reduce(lambda a, b: a + b, [(cols[start] >= 0).astype(jnp.int32) for start, _ in ranges[1:]])
    for kept in (False, True):
        for k, block in enumerate(blocks_of(place, kept)):
            at = rows_of(block, rows)
            scale = [acol[t, at, :] for t in range(bins)]
            for r, (start, count) in enumerate(ranges):
                out = outs[4 * r + 2 * kept + k]
                for i in range(count):
                    for h in range(halves):
                        lanes = slice(h * LANES, (h + 1) * LANES)
                        acc = None
                        for t in range(bins):
                            q = t * halves + h
                            part = trips[t, start + i, at, lanes].astype(F32) * scale[t]
                            part = part * gain[q, start + i : start + i + 1, :]
                            acc = part if acc is None else acc + part
                        out[i, :, lanes] = acc


def factor_kernel(place, cols, target, *refs, start):
    ins, outs = refs[:-2], refs[-2:]
    count, rows, _ = outs[0].shape
    for k, block in enumerate(blocks_of(place, True)):
        for i in range(count):
            empty = (cols[start + i] < 0).astype(F32)
            wanted = target[start + i, rows_of(block, rows), :].astype(F32)
            outs[k][i] = wanted / (ins[2 * k][i] + ins[2 * k + 1][i] + empty)


def fit_kernel(place, trips, acol, gain, fa, fb, sums_in, *refs, start, kept, fill):
    fitted, sums, local, done = refs[-4:]
    bins, slots, side, _ = trips.shape
    halves = side // LANES
    count, rows, _ = fa.shape
    sums[...] = sums_in[...]
    copies = []
    blocks = blocks_of(place, kept)
    places = [rows_of(block, rows) for block in blocks]
    scale = [[acol[t, at, :] for t in range(bins)] for at in places]
    if fill:
        local[:, count] = jnp.zeros((bins, 2, rows, side), local.dtype)
    for i in range(count + fill):
        if i < count:
            for t in range(bins):
                for h in range(halves):
                    lanes = slice(h * LANES, (h + 1) * LANES)
                    q = t * halves + h
                    g = gain[q, start + i : start + i + 1, :]
                    total = None
                    for k, (at, factor) in enumerate(zip(places, (fa, fb))):
                        value = trips[t, start + i, at, lanes].astype(F32) * scale[k][t] * g * factor[i, :, lanes]
                        local[t, i, k, :, lanes] = value.astype(local.dtype)
                        part = jnp.sum(value, axis=0, keepdims=True)
                        total = part if total is None else total + part
                    row = q * slots + start + i
                    sums[row : row + 1, :] = sums[row : row + 1, :] + total
        for k, at in enumerate(places):
            copy = pltpu.make_async_copy(
                local.at[:, min(i, count), k], fitted.at[:, start + i, at, :], done.at[2 * i + k]
            )
            copy.start()
            copies.append(copy)
    for copy in copies:
        copy.wait()


def cycle(trips, acol, gain, target, cols, place, fitted, days, *, ranges):
    bins, slots, side, _ = trips.shape
    halves = side // LANES
    rows = side // 4
    parts = bins * halves
    used = sum(count for _, count in ranges)
    groups = ranges[::-1]
    days = [days[4 * r : 4 * r + 4] for r in range(len(ranges))][::-1]

    def over_first(x):
        return lax.ppermute(x, "tm", [(i, i ^ 2) for i in range(4)])

    def over_second(x):
        return lax.ppermute(x, "tm", [(i, i ^ 1) for i in range(4)])

    def factor(start, count, *sums):
        shape = pltpu.VMEM((count, rows, side), F32)
        return pl.pallas_call(
            functools.partial(factor_kernel, start=start),
            compiler_params=LIMIT,
            in_specs=[whole(pltpu.SMEM)] * 2 + [whole()] * 5,
            out_specs=[whole(), whole()],
            out_shape=[shape, shape],
        )(place, cols, *near(target, *sums))

    def fit(start, count, kept, fill, fa, fb, sums, fitted):
        return pl.pallas_call(
            functools.partial(fit_kernel, start=start, kept=kept, fill=fill),
            compiler_params=LIMIT,
            in_specs=[whole(pltpu.SMEM)] + [whole()] * 6 + [whole(pltpu.HBM)],
            out_specs=[whole(pltpu.HBM), whole()],
            out_shape=[
                pltpu.HBM(trips.shape, trips.dtype),
                pltpu.VMEM((parts * slots, LANES), F32),
            ],
            scratch_shapes=[
                pltpu.VMEM((bins, count + (fill > 0), 2, rows, side), trips.dtype),
                pltpu.SemaphoreType.DMA((2 * (count + fill),)),
            ],
            input_output_aliases={7: 0},
        )(place, *near(trips, acol, gain, fa, fb, sums), pltpu.with_memory_space_constraint(fitted, pltpu.HBM))

    got = [(over_first(d[0]), over_second(d[1])) for d in days]
    mine = [(d[2] + g[0], d[3] + g[1]) for d, g in zip(days, got)]
    other = [(over_second(a), over_first(b)) for a, b in mine]
    scale = [factor(s, n, m[0], o[0], m[1], o[1]) for (s, n), m, o in zip(groups, mine, other)]
    back = [(over_first(a), over_second(b)) for a, b in scale]
    sums = jnp.zeros((parts * slots, LANES), F32)
    for (s, n), f, b in zip(groups, scale, back):
        fill = slots - used if s + n == used else 0
        fitted, sums = fit(s, n, True, fill, f[0], f[1], sums, fitted)
        fitted, sums = fit(s, n, False, fill, b[0], b[1], sums, fitted)
    return fitted, sums


def empty_kernel(out):
    pass


def gather(x, n, beside):
    def swap(y, k):
        return lax.ppermute(y, "orig", [(i, i ^ k) for i in range(n)])

    far = [swap(x, k) for k in range(n - 2, 0, -2)]
    if beside is not None:
        far, beside = lax.optimization_barrier((far, beside))
    close = jnp.stack([x] + far)
    return [close, swap(close, 1)], beside


def make(mesh):
    n_orig = mesh.shape["orig"]
    n_tm = mesh.shape["tm"]
    assert n_tm == 4 and n_orig & (n_orig - 1) == 0 and n_orig > 1

    def on_device(trip_counts, anchor_hour, dest_hour, daily_target, block_columns):
        bins, slots, side, _ = trip_counts.shape
        halves = side // LANES
        parts = bins * halves
        width = dest_hour.shape[1] // n_orig
        place = jnp.stack([lax.axis_index("tm").astype(jnp.int32), lax.axis_index("orig").astype(jnp.int32)])
        place, block_columns = lax.optimization_barrier((place, block_columns))

        local, acol, sums = pl.pallas_call(
            anchor_kernel,
            compiler_params=LIMIT,
            in_specs=[whole(pltpu.SMEM), whole(pltpu.SMEM), whole(), whole(pltpu.HBM)],
            out_specs=[whole(), whole(), whole()],
            out_shape=[
                pltpu.VMEM(trip_counts.shape, trip_counts.dtype),
                pltpu.VMEM((bins, side, LANES), F32),
                pltpu.VMEM(((parts + 1) * slots, LANES), F32),
            ],
            scratch_shapes=[pltpu.SemaphoreType.DMA((bins,))],
        )(place, block_columns, anchor_hour, pltpu.with_memory_space_constraint(trip_counts, pltpu.HBM))

        picked, span = pl.pallas_call(
            lookup_kernel,
            compiler_params=LIMIT,
            in_specs=[whole(pltpu.SMEM), whole(pltpu.SMEM), whole()],
            out_specs=[whole(), whole()],
            out_shape=[
                pltpu.VMEM((parts, slots, LANES), F32),
                pltpu.VMEM((bins, width), F32),
            ],
        )(place, block_columns, dest_hour)
        arrived, picked = gather(sums, n_orig, picked)

        gain, columns = pl.pallas_call(
            gain_kernel,
            compiler_params=LIMIT,
            in_specs=[whole()] * (1 + len(arrived)),
            out_specs=[whole(), whole()],
            out_shape=[
                pltpu.VMEM((parts, slots, LANES), F32),
                pltpu.VMEM((n_orig, slots, LANES), F32),
            ],
        )(*near(picked, *arrived))

        blank = pl.pallas_call(
            empty_kernel,
            compiler_params=LIMIT,
            out_specs=whole(pltpu.HBM),
            out_shape=pltpu.HBM(trip_counts.shape, trip_counts.dtype),
        )()

        cuts = [max(slots // 6, 1), max(slots // 2, 2), slots]
        ranges = [(a, b - a) for a, b in zip([0] + cuts, cuts)]
        quarter = side // 4
        *days, pick = pl.pallas_call(
            functools.partial(day_kernel, ranges=ranges),
            compiler_params=LIMIT,
            in_specs=[whole(pltpu.SMEM)] * 2 + [whole()] * 3,
            out_specs=[whole()] * (4 * len(ranges)) + [whole(pltpu.SMEM)],
            out_shape=[pltpu.VMEM((n, quarter, side), F32) for _, n in ranges for _ in range(4)]
            + [jax.ShapeDtypeStruct((1,), jnp.int32)],
        )(place, block_columns, *near(local, acol, gain))
        fitted, final = lax.switch(
            pick[0],
            [functools.partial(cycle, ranges=ranges[: k + 1]) for k in range(len(ranges))],
            local,
            acol,
            gain,
            daily_target,
            block_columns,
            place,
            blank,
            days,
        )
        finals, _ = gather(final, n_orig, None)
        gap = pl.pallas_call(
            gap_kernel,
            compiler_params=LIMIT,
            in_specs=[whole(pltpu.SMEM), whole(), whole()] + [whole()] * len(finals),
            out_specs=whole(),
            out_shape=jax.ShapeDtypeStruct((bins, width), F32),
        )(place, *near(span, columns, *finals))
        return fitted, gap

    return on_device


def solution(mesh):
    placed = (
        P("tm", "orig", None, None),
        P("tm", "orig"),
        P("tm", None),
        P("orig", None, None),
        P("orig"),
    )
    return jax.shard_map(
        make(mesh),
        mesh=mesh,
        in_specs=placed,
        out_specs=(P("tm", "orig", None, None), P("tm", "orig")),
        check_vma=False,
    )
```

```python
import functools

import jax
import jax.numpy as jnp
from jax import lax
from jax.experimental import pallas as pl
from jax.experimental.pallas import tpu as pltpu
from jax.sharding import PartitionSpec as P


LANES = 128
F32 = jnp.float32
LIMIT = pltpu.CompilerParams(vmem_limit_bytes=8 * 2**20)


def whole(memory_space=pltpu.VMEM):
    return pl.BlockSpec(memory_space=memory_space)


def near(*xs):
    return [pltpu.with_memory_space_constraint(x, pltpu.VMEM) for x in xs]


def far(*xs):
    return [pltpu.with_memory_space_constraint(x, pltpu.HBM) for x in xs]


def anchor_kernel(place, cols, anchor, trips, local, acol, sums, pick, margins, arrivals, *, starts):
    bins, slots, side, _ = trips.shape
    halves = side // LANES
    rows = side // 4
    first = pltpu.make_async_copy(anchor, margins, arrivals.at[4 * bins])
    first.start()
    blocks = [(t, r) for t in range(bins) for r in range(0, side, rows)]
    copies = [
        pltpu.make_async_copy(trips.at[t, :, r : r + rows, :], local.at[t, :, r : r + rows, :], arrivals.at[i])
        for i, (t, r) in enumerate(blocks)
    ]
    for copy in copies:
        copy.start()
    pick[0] = functools.reduce(lambda a, b: a + b, [(cols[s] >= 0).astype(jnp.int32) for s in starts])
    count = bins * halves * slots
    for s in range(slots):
        sums[count + s : count + s + 1, :] = jnp.full((1, LANES), cols[s], jnp.int32).astype(F32)
    live = [(cols[s] >= 0).astype(F32) for s in range(slots)]
    first.wait()
    acc = None
    for copy, (t, r) in zip(copies, blocks):
        copy.wait()
        if r == 0:
            acc = [[None] * halves for _ in range(slots)]
        total = None
        for s in range(slots):
            part = local[t, s, r : r + rows, :].astype(F32) * live[s]
            total = part if total is None else total + part
        total = jnp.sum(total, axis=1, keepdims=True)
        diagonal = (
            lax.broadcasted_iota(jnp.int32, (rows, side), 0) + r == lax.broadcasted_iota(jnp.int32, (rows, side), 1)
        )
        column = jnp.sum(jnp.where(diagonal, margins[t : t + 1, :], 0.0), axis=1, keepdims=True)
        scale = jnp.broadcast_to(column / total, (rows, LANES))
        acol[t, r : r + rows, :] = scale
        for s in range(slots):
            for h in range(halves):
                part = local[t, s, r : r + rows, h * LANES : (h + 1) * LANES].astype(F32) * scale
                part = jnp.sum(part.reshape(rows // 8, 8, LANES), axis=0)
                acc[s][h] = part if acc[s][h] is None else acc[s][h] + part
        if r + rows == side:
            for h in range(halves):
                for s in range(slots):
                    row = (t * halves + h) * slots + s
                    sums[row : row + 1, :] = jnp.sum(acc[s][h], axis=0, keepdims=True)


def lookup_kernel(place, cols, dest, picked, span):
    parts, slots, _ = picked.shape
    bins = dest.shape[0]
    halves = parts // bins
    side = halves * LANES
    for s in range(slots):
        start = pl.multiple_of(jnp.maximum(cols[s], 0) * side, side)
        row = dest[:, pl.ds(start, side)]
        for t in range(bins):
            for h in range(halves):
                picked[t * halves + h, s : s + 1, :] = row[t : t + 1, h * LANES : (h + 1) * LANES]
    width = span.shape[1]
    span[...] = dest[:, pl.ds(pl.multiple_of(place[1] * width, width), width)]


def matched(own, columns, values, parts, slots, first):
    acc = [jnp.zeros(own.shape, F32) for _ in range(parts)]
    at = 0
    for vref in values:
        for k in range(vref.shape[0]):
            cref, c = (vref, k) if columns is None else (columns, at)
            at += 1
            for s in range(slots):
                hit = own == cref[c, first + s : first + s + 1, :]
                for q in range(parts):
                    acc[q] = acc[q] + jnp.where(hit, vref[k, q * slots + s : q * slots + s + 1, :], 0.0)
    return acc


def gap_kernel(place, span, *refs):
    out = refs[-1]
    columns, values = refs[0], refs[1:-1]
    slots = columns.shape[1]
    first = values[0].shape[1]
    parts = first // slots
    bins = out.shape[0]
    halves = parts // bins
    side = halves * LANES
    blocks = out.shape[1] // side
    own = (lax.broadcasted_iota(jnp.int32, (blocks, LANES), 0) + place[1] * blocks).astype(F32)
    total = matched(own, columns, values, parts, slots, 0)
    for t in range(bins):
        for h in range(halves):
            for c in range(blocks):
                at = c * side + h * LANES
                out[t : t + 1, at : at + LANES] = total[t * halves + h][c : c + 1, :]
    out[...] = out[...] / span[...] - 1.0


def blocks_of(place, kept):
    first, second = place[0] >> 1, place[0] & 1
    if kept:
        return first, 2 + second
    return 1 - first, 3 - second


def rows_of(block, rows):
    return pl.ds(pl.multiple_of(block * rows, rows), rows)


def day_kernel(place, trips, acol, picked, *refs, ranges, count):
    arrived, gain, columns, outs = refs[:count], refs[count], refs[count + 1], refs[count + 2 :]
    bins, slots, side, _ = trips.shape
    halves = side // LANES
    rows = side // 4
    parts = bins * halves
    first = parts * slots
    own = arrived[0][0, first : first + slots, :]
    total = matched(own, None, arrived, parts, slots, first)
    for q in range(parts):
        gain[q] = jnp.where(own >= 0.0, picked[q] / jnp.maximum(total[q], 1.0), 0.0)
    at = 0
    for ref in arrived:
        for k in range(ref.shape[0]):
            columns[at] = ref[k, first : first + slots, :]
            at += 1
    for kept in (False, True):
        for k, block in enumerate(blocks_of(place, kept)):
            at = rows_of(block, rows)
            scale = [acol[t, at, :] for t in range(bins)]
            for r, (start, n) in enumerate(ranges):
                out = outs[4 * r + 2 * kept + k]
                for i in range(n):
                    for h in range(halves):
                        lanes = slice(h * LANES, (h + 1) * LANES)
                        acc = None
                        for t in range(bins):
                            q = t * halves + h
                            part = trips[t, start + i, at, lanes].astype(F32) * scale[t]
                            part = part * gain[q, start + i : start + i + 1, :]
                            acc = part if acc is None else acc + part
                        out[i, :, lanes] = acc


def factor_kernel(place, cols, target, *refs, start):
    ins, outs = refs[:-2], refs[-2:]
    count, rows, _ = outs[0].shape
    for k, block in enumerate(blocks_of(place, True)):
        for i in range(count):
            empty = (cols[start + i] < 0).astype(F32)
            wanted = target[start + i, rows_of(block, rows), :].astype(F32)
            outs[k][i] = wanted / (ins[2 * k][i] + ins[2 * k + 1][i] + empty)


def fit_rows(place, trips, acol, gain, fa, fb, sums_in, local, sums, start, kept):
    bins, slots, side, _ = trips.shape
    halves = side // LANES
    count, rows, _ = fa.shape
    sums[...] = sums_in[...]
    places = [rows_of(block, rows) for block in blocks_of(place, kept)]
    scale = [[acol[t, at, :] for t in range(bins)] for at in places]
    for i in range(count):
        for t in range(bins):
            for h in range(halves):
                lanes = slice(h * LANES, (h + 1) * LANES)
                q = t * halves + h
                g = gain[q, start + i : start + i + 1, :]
                total = None
                for k, (at, factor) in enumerate(zip(places, (fa, fb))):
                    value = trips[t, start + i, at, lanes].astype(F32) * scale[k][t] * g * factor[i, :, lanes]
                    local[t, i, at, lanes] = value.astype(local.dtype)
                    part = jnp.sum(value.reshape(rows // 8, 8, LANES), axis=0)
                    total = part if total is None else total + part
                row = q * slots + start + i
                sums[row : row + 1, :] = sums[row : row + 1, :] + jnp.sum(total, axis=0, keepdims=True)


def kept_kernel(place, trips, acol, gain, fa, fb, sums_in, local, sums, *, start):
    fit_rows(place, trips, acol, gain, fa, fb, sums_in, local, sums, start, True)


def rest_kernel(place, trips, acol, gain, fa, fb, sums_in, mine, *refs, start, before, empty, last, chained):
    refs = list(refs)
    ready = refs.pop(0) if before is not None else None
    if chained:
        refs.pop(0)
    local, sums = refs[:2]
    fitted, blank, done = refs[2:] if len(refs) > 2 else (None, None, None)
    bins, count, _, _ = local.shape
    copies = []

    def put(source, target):
        copies.append(pltpu.make_async_copy(source, target, done.at[len(copies)]))
        copies[-1].start()

    if empty:
        blank[...] = jnp.zeros(blank.shape, blank.dtype)
    for t in range(bins):
        if before is not None:
            put(ready.at[t], fitted.at[t, before[0] : before[0] + before[1]])
        for s in empty:
            put(blank, fitted.at[t, s])
    fit_rows(place, trips, acol, gain, fa, fb, sums_in, local, sums, start, False)
    if last:
        for t in range(bins):
            put(local.at[t], fitted.at[t, start : start + count])
    for copy in copies:
        copy.wait()


def cycle(trips, acol, gain, target, cols, place, days, *, ranges):
    bins, slots, side, _ = trips.shape
    halves = side // LANES
    rows = side // 4
    parts = bins * halves
    used = sum(count for _, count in ranges)
    groups = ranges[::-1]
    days = [days[4 * r : 4 * r + 4] for r in range(len(ranges))][::-1]

    def over_first(x):
        return lax.ppermute(x, "tm", [(i, i ^ 2) for i in range(4)])

    def over_second(x):
        return lax.ppermute(x, "tm", [(i, i ^ 1) for i in range(4)])

    def factor(start, count, *sums):
        shape = pltpu.VMEM((count, rows, side), F32)
        return pl.pallas_call(
            functools.partial(factor_kernel, start=start),
            compiler_params=LIMIT,
            in_specs=[whole(pltpu.SMEM)] * 2 + [whole()] * 5,
            out_specs=[whole(), whole()],
            out_shape=[shape, shape],
        )(place, cols, *near(target, *sums))

    def fit_kept(start, count, fa, fb, sums):
        return pl.pallas_call(
            functools.partial(kept_kernel, start=start),
            compiler_params=LIMIT,
            in_specs=[whole(pltpu.SMEM)] + [whole()] * 6,
            out_specs=[whole(), whole()],
            out_shape=[pltpu.VMEM((bins, count, side, side), trips.dtype), pltpu.VMEM((parts * slots, LANES), F32)],
        )(place, *near(trips, acol, gain, fa, fb, sums))

    def fit_rest(start, count, fa, fb, sums, mine, before, ready, fitted, last):
        empty = range(used, slots) if fitted is None and before is None else ()
        if len(groups) > 1 and used == slots:
            empty = ()
        writes = before is not None or len(empty) > 0 or last
        extra = near(ready) if before is not None else []
        aliases = {7: 0}
        if fitted is not None:
            aliases[8 + len(extra)] = 2
            extra = extra + far(fitted)
        in_specs = [whole(pltpu.SMEM)] + [whole()] * 7 + [whole()] * (before is not None)
        in_specs += [whole(pltpu.HBM)] * (fitted is not None)
        copies = bins * ((before is not None) + len(empty) + last)
        outs = pl.pallas_call(
            functools.partial(
                rest_kernel, start=start, before=before, empty=empty, last=last, chained=fitted is not None
            ),
            compiler_params=LIMIT,
            in_specs=in_specs,
            out_specs=[whole(), whole()] + [whole(pltpu.HBM)] * writes,
            out_shape=[pltpu.VMEM((bins, count, side, side), trips.dtype), pltpu.VMEM((parts * slots, LANES), F32)]
            + [pltpu.HBM(trips.shape, trips.dtype)] * writes,
            scratch_shapes=[pltpu.VMEM((side, side), trips.dtype), pltpu.SemaphoreType.DMA((copies,))] * writes,
            input_output_aliases=aliases,
        )(place, *near(trips, acol, gain, fa, fb, sums, mine), *extra)
        return outs if writes else [*outs, None]

    order = range(len(groups))
    got = [(over_first(days[g][0]), over_second(days[g][1])) for g in order]
    mine = [(d[2] + g[0], d[3] + g[1]) for d, g in zip(days, got)]
    other = [(over_second(mine[g][0]), over_first(mine[g][1])) for g in order]
    scale = [factor(s, n, m[0], o[0], m[1], o[1]) for (s, n), m, o in zip(groups, mine, other)]
    back = [(over_first(scale[g][0]), over_second(scale[g][1])) for g in order]
    sums = jnp.zeros((parts * slots, LANES), F32)
    before = ready = fitted = None
    for i, ((s, n), f, b) in enumerate(zip(groups, scale, back)):
        local, sums = fit_kept(s, n, f[0], f[1], sums)
        ready, sums, fitted = fit_rest(
            s, n, b[0], b[1], sums, local, before, ready, fitted, i == len(groups) - 1
        )
        before = (s, n)
    return fitted, sums


def gather(x, n, beside):
    def swap(y, k):
        return lax.ppermute(y, "orig", [(i, i ^ k) for i in range(n)])

    distant = [swap(x, k) for k in range(n - 2, 0, -2)]
    distant, beside = lax.optimization_barrier((distant, beside))
    close = jnp.stack([x] + distant)
    return [close, swap(close, 1)], beside


def make(mesh):
    n_orig = mesh.shape["orig"]
    n_tm = mesh.shape["tm"]
    assert n_tm == 4 and n_orig & (n_orig - 1) == 0 and n_orig > 1

    def on_device(trip_counts, anchor_hour, dest_hour, daily_target, block_columns):
        bins, slots, side, _ = trip_counts.shape
        halves = side // LANES
        parts = bins * halves
        width = dest_hour.shape[1] // n_orig
        place = jnp.stack([lax.axis_index("tm").astype(jnp.int32), lax.axis_index("orig").astype(jnp.int32)])
        place, block_columns = lax.optimization_barrier((place, block_columns))

        cuts = [max(slots // 6, 1), max(slots // 2, 2), slots]
        ranges = [(a, b - a) for a, b in zip([0] + cuts, cuts)]
        local, acol, sums, pick = pl.pallas_call(
            functools.partial(anchor_kernel, starts=cuts[:-1]),
            compiler_params=LIMIT,
            in_specs=[whole(pltpu.SMEM), whole(pltpu.SMEM), whole(pltpu.HBM), whole(pltpu.HBM)],
            out_specs=[whole(), whole(), whole(), whole(pltpu.SMEM)],
            out_shape=[
                pltpu.VMEM(trip_counts.shape, trip_counts.dtype),
                pltpu.VMEM((bins, side, LANES), F32),
                pltpu.VMEM(((parts + 1) * slots, LANES), F32),
                jax.ShapeDtypeStruct((1,), jnp.int32),
            ],
            scratch_shapes=[pltpu.VMEM((bins, side), F32), pltpu.SemaphoreType.DMA((4 * bins + 1,))],
        )(place, block_columns, *far(anchor_hour, trip_counts))

        picked, span = pl.pallas_call(
            lookup_kernel,
            compiler_params=LIMIT,
            in_specs=[whole(pltpu.SMEM), whole(pltpu.SMEM), whole()],
            out_specs=[whole(), whole()],
            out_shape=[
                pltpu.VMEM((parts, slots, LANES), F32),
                pltpu.VMEM((bins, width), F32),
            ],
        )(place, block_columns, dest_hour)
        arrived, picked = gather(sums, n_orig, picked)

        quarter = side // 4
        gain, columns, *days = pl.pallas_call(
            functools.partial(day_kernel, ranges=ranges, count=len(arrived)),
            compiler_params=LIMIT,
            in_specs=[whole(pltpu.SMEM)] + [whole()] * (3 + len(arrived)),
            out_specs=[whole()] * (2 + 4 * len(ranges)),
            out_shape=[
                pltpu.VMEM((parts, slots, LANES), F32),
                pltpu.VMEM((n_orig, slots, LANES), F32),
            ]
            + [pltpu.VMEM((n, quarter, side), F32) for _, n in ranges for _ in range(4)],
        )(place, *near(local, acol, picked, *arrived))

        def branch(k):
            def run(*args):
                return cycle(*args, ranges=ranges[: k + 1])

            return run

        days, pick = lax.optimization_barrier((days, pick))
        fitted, final = lax.switch(
            pick[0],
            [branch(k) for k in range(len(ranges))],
            local,
            acol,
            gain,
            daily_target,
            block_columns,
            place,
            days,
        )
        fitted, final = lax.optimization_barrier((fitted, final))
        finals, _ = gather(final, n_orig, place)
        gap = pl.pallas_call(
            gap_kernel,
            compiler_params=LIMIT,
            in_specs=[whole(pltpu.SMEM), whole(), whole()] + [whole()] * len(finals),
            out_specs=whole(),
            out_shape=jax.ShapeDtypeStruct((bins, width), F32),
        )(place, *near(span, columns, *finals))
        return fitted, gap

    return on_device


def solution(mesh):
    placed = (
        P("tm", "orig", None, None),
        P("tm", "orig"),
        P("tm", None),
        P("orig", None, None),
        P("orig"),
    )
    return jax.shard_map(
        make(mesh),
        mesh=mesh,
        in_specs=placed,
        out_specs=(P("tm", "orig", None, None), P("tm", "orig")),
        check_vma=False,
    )
```

```python
import functools

import jax
import jax.numpy as jnp
from jax import lax
from jax.experimental import pallas as pl
from jax.experimental.pallas import tpu as pltpu
from jax.sharding import PartitionSpec as P


LANES = 128
F32 = jnp.float32
LIMIT = pltpu.CompilerParams(vmem_limit_bytes=8 * 2**20)


def whole(memory_space=pltpu.VMEM):
    return pl.BlockSpec(memory_space=memory_space)


def near(*xs):
    return [pltpu.with_memory_space_constraint(x, pltpu.VMEM) for x in xs]


def far(*xs):
    return [pltpu.with_memory_space_constraint(x, pltpu.HBM) for x in xs]


def anchor_kernel(place, cols, anchor, trips, local, acol, sums, pick, margins, arrivals, *, starts):
    bins, slots, side, _ = trips.shape
    halves = side // LANES
    rows = side // 4
    first = pltpu.make_async_copy(anchor, margins, arrivals.at[4 * bins])
    first.start()
    blocks = [(t, r) for t in range(bins) for r in range(0, side, rows)]
    copies = [
        pltpu.make_async_copy(trips.at[t, :, r : r + rows, :], local.at[t, :, r : r + rows, :], arrivals.at[i])
        for i, (t, r) in enumerate(blocks)
    ]
    for copy in copies:
        copy.start()
    pick[0] = functools.reduce(lambda a, b: a + b, [(cols[s] >= 0).astype(jnp.int32) for s in starts])
    count = bins * halves * slots
    for s in range(slots):
        sums[count + s : count + s + 1, :] = jnp.full((1, LANES), cols[s], jnp.int32).astype(F32)
    live = [(cols[s] >= 0).astype(F32) for s in range(slots)]
    first.wait()
    for t, r in blocks:
        diagonal = (
            lax.broadcasted_iota(jnp.int32, (rows, side), 0) + r == lax.broadcasted_iota(jnp.int32, (rows, side), 1)
        )
        column = jnp.sum(jnp.where(diagonal, margins[t : t + 1, :], 0.0), axis=1, keepdims=True)
        acol[t, r : r + rows, :] = jnp.broadcast_to(column, (rows, LANES))

    def row_totals(t, r):
        total = None
        for s in range(slots):
            part = local[t, s, r : r + rows, :].astype(F32) * live[s]
            total = part if total is None else total + part
        return jnp.sum(total, axis=1, keepdims=True)

    def column_sums(t, r, total, acc):
        scale = acol[t, r : r + rows, :] / jnp.broadcast_to(total, (rows, LANES))
        acol[t, r : r + rows, :] = scale
        for s in range(slots):
            for h in range(halves):
                part = local[t, s, r : r + rows, h * LANES : (h + 1) * LANES].astype(F32) * scale
                part = jnp.sum(part.reshape(rows // 8, 8, LANES), axis=0)
                acc[s][h] = part if r == 0 else acc[s][h] + part
        if r + rows == side:
            for h in range(halves):
                for s in range(slots):
                    row = (t * halves + h) * slots + s
                    sums[row : row + 1, :] = jnp.sum(acc[s][h], axis=0, keepdims=True)

    acc = [[None] * halves for _ in range(slots)]
    waiting = None
    for copy, (t, r) in zip(copies, blocks):
        copy.wait()
        total = row_totals(t, r)
        if waiting is not None:
            column_sums(*waiting, acc)
        waiting = (t, r, total)
    column_sums(*waiting, acc)


def lookup_kernel(place, cols, dest, target, picked, span, *wanted, ranges):
    parts, slots, _ = picked.shape
    bins = dest.shape[0]
    halves = parts // bins
    side = halves * LANES
    for s in range(slots):
        start = pl.multiple_of(jnp.maximum(cols[s], 0) * side, side)
        row = dest[:, pl.ds(start, side)]
        for t in range(bins):
            for h in range(halves):
                picked[t * halves + h, s : s + 1, :] = row[t : t + 1, h * LANES : (h + 1) * LANES]
    width = span.shape[1]
    span[...] = dest[:, pl.ds(pl.multiple_of(place[1] * width, width), width)]
    for r, (start, count) in enumerate(ranges):
        for k, block in enumerate(blocks_of(place, True)):
            out = wanted[2 * r + k]
            out[...] = target[start : start + count, rows_of(block, out.shape[1]), :].astype(F32)


def matched(own, columns, values, parts, slots, first):
    acc = [jnp.zeros(own.shape, F32) for _ in range(parts)]
    at = 0
    for vref in values:
        for k in range(vref.shape[0]):
            cref, c = (vref, k) if columns is None else (columns, at)
            at += 1
            for s in range(slots):
                hit = own == cref[c, first + s : first + s + 1, :]
                for q in range(parts):
                    acc[q] = acc[q] + jnp.where(hit, vref[k, q * slots + s : q * slots + s + 1, :], 0.0)
    return acc


def gap_kernel(place, span, *refs):
    out = refs[-1]
    columns, values = refs[0], refs[1:-1]
    slots = columns.shape[1]
    first = values[0].shape[1]
    parts = first // slots
    bins = out.shape[0]
    halves = parts // bins
    side = halves * LANES
    blocks = out.shape[1] // side
    own = (lax.broadcasted_iota(jnp.int32, (blocks, LANES), 0) + place[1] * blocks).astype(F32)
    total = matched(own, columns, values, parts, slots, 0)
    for t in range(bins):
        for h in range(halves):
            for c in range(blocks):
                at = c * side + h * LANES
                out[t : t + 1, at : at + LANES] = total[t * halves + h][c : c + 1, :]
    out[...] = out[...] / span[...] - 1.0


def blocks_of(place, kept):
    first, second = place[0] >> 1, place[0] & 1
    if kept:
        return first, 2 + second
    return 1 - first, 3 - second


def rows_of(block, rows):
    return pl.ds(pl.multiple_of(block * rows, rows), rows)


def day_kernel(place, trips, acol, picked, *refs, ranges, count):
    arrived, gain, columns, first_trips, outs = refs[:count], refs[count], refs[count + 1], refs[count + 2], refs[count + 3 :]
    first_trips[...] = trips[:, : first_trips.shape[1]]
    bins, slots, side, _ = trips.shape
    halves = side // LANES
    parts = bins * halves
    first = parts * slots
    own = arrived[0][0, first : first + slots, :]
    total = matched(own, None, arrived, parts, slots, first)
    for q in range(parts):
        gain[q] = jnp.where(own >= 0.0, picked[q] / jnp.maximum(total[q], 1.0), 0.0)
    at = 0
    for ref in arrived:
        for k in range(ref.shape[0]):
            columns[at] = ref[k, first : first + slots, :]
            at += 1
    day_parts(place, trips, acol, gain, outs, ranges, False)


def keep_kernel(place, trips, acol, gain, *outs, ranges):
    day_parts(place, trips, acol, gain, outs, ranges, True)


def day_parts(place, trips, acol, gain, outs, ranges, kept):
    bins, _, side, _ = trips.shape
    halves = side // LANES
    rows = side // 4
    for k, block in enumerate(blocks_of(place, kept)):
        at = rows_of(block, rows)
        scale = [acol[t, at, :] for t in range(bins)]
        for r, (start, n) in enumerate(ranges):
            out = outs[2 * r + k]
            for i in range(n):
                for h in range(halves):
                    lanes = slice(h * LANES, (h + 1) * LANES)
                    acc = None
                    for t in range(bins):
                        q = t * halves + h
                        part = trips[t, start + i, at, lanes].astype(F32) * scale[t]
                        part = part * gain[q, start + i : start + i + 1, :]
                        acc = part if acc is None else acc + part
                    out[i, :, lanes] = acc


def fit_rows(place, trips, acol, gain, fa, fb, local, sums, start, kept):
    bins, _, side, _ = trips.shape
    slots = gain.shape[1]
    halves = side // LANES
    count, rows, _ = fa.shape
    places = [rows_of(block, rows) for block in blocks_of(place, kept)]
    scale = [[acol[t, at, :] for t in range(bins)] for at in places]
    for i in range(count):
        for t in range(bins):
            for h in range(halves):
                lanes = slice(h * LANES, (h + 1) * LANES)
                q = t * halves + h
                g = gain[q, start + i : start + i + 1, :]
                total = None
                for k, (at, factor) in enumerate(zip(places, (fa, fb))):
                    value = trips[t, start + i, at, lanes].astype(F32) * scale[k][t] * g * factor[i, :, lanes]
                    local[t, i, at, lanes] = value.astype(local.dtype)
                    part = jnp.sum(value.reshape(rows // 8, 8, LANES), axis=0)
                    total = part if total is None else total + part
                row = q * slots + start + i
                total = jnp.sum(total, axis=0, keepdims=True)
                sums[row : row + 1, :] = total if kept else sums[row : row + 1, :] + total


def copy_all(pairs, done):
    copies = [pltpu.make_async_copy(source, target, done.at[i]) for i, (source, target) in enumerate(pairs)]
    for copy in copies:
        copy.start()
    return copies


def copy_all(pairs, done, first=0):
    copies = [pltpu.make_async_copy(source, target, done.at[first + i]) for i, (source, target) in enumerate(pairs)]
    for copy in copies:
        copy.start()
    return copies


def empty_kernel(sums, fitted, blank, done, *, empty):
    sums[...] = jnp.zeros(sums.shape, F32)
    blank[...] = jnp.zeros(blank.shape, blank.dtype)
    for copy in copy_all([(blank, fitted.at[t, s]) for t in range(fitted.shape[0]) for s in empty], done):
        copy.wait()


def kept_kernel(place, trips, acol, gain, sums_in, *refs, ranges):
    n = len(ranges)
    factors, locals_, sums = refs[: 2 * n], refs[2 * n : 3 * n], refs[3 * n]
    sums[...] = sums_in[...]
    for r, (start, _) in enumerate(ranges):
        fit_rows(place, trips, acol, gain, factors[2 * r], factors[2 * r + 1], locals_[r], sums, start, True)


def rest_kernel(place, trips, acol, gain, fa, fb, sums_in, mine, *refs, start, ready_start, chained, last):
    refs = list(refs)
    ready = refs.pop(0) if ready_start is not None else None
    if chained:
        refs.pop(0)
    local, sums = refs[:2]
    bins, count, _, _ = local.shape
    copies = []
    if ready is not None:
        fitted, done = refs[2:]
        pairs = [(ready.at[t], fitted.at[t, ready_start : ready_start + ready.shape[1]]) for t in range(bins)]
        copies += copy_all(pairs, done)
    sums[...] = sums_in[...]
    fit_rows(place, trips, acol, gain, fa, fb, local, sums, start, False)
    if last:
        fitted, done = refs[2:]
        copies += copy_all([(local.at[t], fitted.at[t, start : start + count]) for t in range(bins)], done, len(copies))
    for copy in copies:
        copy.wait()


def end_kernel(place, trips, acol, gain, fa, fb, ga, gb, sums_in, local, sums, *, start):
    sums[...] = sums_in[...]
    fit_rows(place, trips, acol, gain, fa, fb, local, sums, start, True)
    fit_rows(place, trips, acol, gain, ga, gb, local, sums, start, False)


def store_kernel(local, before, fitted, done, *, start):
    bins, count, _, _ = local.shape
    for copy in copy_all([(local.at[t], fitted.at[t, start : start + count]) for t in range(bins)], done):
        copy.wait()


def cycle(trips, acol, gain, cols, place, wanted, sends, *, ranges, used):
    bins, slots, side, _ = trips.shape
    halves = side // LANES
    rows = side // 4
    parts = bins * halves
    order = range(used)[::-1]

    def over_first(x):
        return lax.ppermute(x, "tm", [(i, i ^ 2) for i in range(4)])

    def over_second(x):
        return lax.ppermute(x, "tm", [(i, i ^ 1) for i in range(4)])

    def factor(r, k, mine, other):
        start, count = ranges[r]
        empty = (cols[start : start + count] < 0).astype(F32)[:, None, None]
        return wanted[2 * r + k] / (mine + other + empty)

    def total(kept, got):
        return kept + got

    got = {r: (over_first(sends[2 * r]), over_second(sends[2 * r + 1])) for r in order}
    kept = pl.pallas_call(
        functools.partial(keep_kernel, ranges=ranges[:used]),
        compiler_params=LIMIT,
        in_specs=[whole(pltpu.SMEM)] + [whole()] * 3,
        out_specs=[whole()] * (2 * used),
        out_shape=[pltpu.VMEM((n, rows, side), F32) for _, n in ranges[:used] for _ in range(2)],
    )(place, *near(trips, acol, gain))
    mine = {r: [total(kept[2 * r + k], got[r][k]) for k in range(2)] for r in order}
    other = {r: (over_second(mine[r][0]), over_first(mine[r][1])) for r in order}
    scale = {r: [factor(r, k, mine[r][k], other[r][k]) for k in range(2)] for r in order}
    back = {r: (over_first(scale[r][0]), over_second(scale[r][1])) for r in order}
    shapes = [pltpu.VMEM((bins, n, side, side), trips.dtype) for _, n in ranges]
    final = pltpu.VMEM((parts * slots, LANES), F32)
    store = pltpu.HBM(trips.shape, trips.dtype)
    sums, fitted = jnp.zeros((parts * slots, LANES), F32), None
    if used < len(ranges):
        empty = range(ranges[used][0], slots)
        sums, fitted = pl.pallas_call(
            functools.partial(empty_kernel, empty=empty),
            compiler_params=LIMIT,
            out_specs=[whole(), whole(pltpu.HBM)],
            out_shape=[final, store],
            scratch_shapes=[pltpu.VMEM((side, side), trips.dtype), pltpu.SemaphoreType.DMA((bins * len(empty),))],
        )()
    if used > 1:
        *out, sums = pl.pallas_call(
            functools.partial(kept_kernel, ranges=ranges[1:used]),
            compiler_params=LIMIT,
            in_specs=[whole(pltpu.SMEM)] + [whole()] * (4 + 2 * (used - 1)),
            out_specs=[whole()] * used,
            out_shape=[*shapes[1:used], final],
        )(place, *near(trips, acol, gain, sums, *[f for r in range(1, used) for f in scale[r]]))
        out = [None] + out
    for r in order[:-1]:
        ready = [out[r + 1]] if r + 1 < used else []
        last = r == 1
        writes = len(ready) + last
        chain = far(fitted) if writes and fitted is not None else []
        outs = pl.pallas_call(
            functools.partial(
                rest_kernel,
                start=ranges[r][0],
                ready_start=ranges[r + 1][0] if ready else None,
                chained=len(chain) > 0,
                last=last,
            ),
            compiler_params=LIMIT,
            in_specs=[whole(pltpu.SMEM)] + [whole()] * (7 + len(ready)) + [whole(pltpu.HBM)] * len(chain),
            out_specs=[whole(), whole()] + [whole(pltpu.HBM)] * (writes > 0),
            out_shape=[shapes[r], final] + [store] * (writes > 0),
            scratch_shapes=[pltpu.SemaphoreType.DMA((bins * writes,))] * (writes > 0),
            input_output_aliases={7: 0} | ({8 + len(ready): 2} if chain else {}),
        )(place, *near(trips, acol, gain, *back[r], sums, out[r], *ready), *chain)
        out[r], sums = outs[:2]
        if writes:
            fitted = outs[2]
    return [*scale[0], *back[0]], sums, fitted


def gather(x, n, beside):
    def swap(y, k):
        return lax.ppermute(y, "orig", [(i, i ^ k) for i in range(n)])

    distant = [swap(x, k) for k in range(n - 2, 0, -2)]
    distant, beside = lax.optimization_barrier((distant, beside))
    close = jnp.stack([x] + distant)
    return [close, swap(close, 1)], beside


def make(mesh):
    n_orig = mesh.shape["orig"]
    n_tm = mesh.shape["tm"]
    assert n_tm == 4 and n_orig & (n_orig - 1) == 0 and n_orig > 1

    def on_device(trip_counts, anchor_hour, dest_hour, daily_target, block_columns):
        bins, slots, side, _ = trip_counts.shape
        halves = side // LANES
        parts = bins * halves
        width = dest_hour.shape[1] // n_orig
        place = jnp.stack([lax.axis_index("tm").astype(jnp.int32), lax.axis_index("orig").astype(jnp.int32)])
        place, block_columns = lax.optimization_barrier((place, block_columns))

        cuts = [max(slots // 6, 1), max(slots // 2, 2), slots]
        ranges = [(a, b - a) for a, b in zip([0] + cuts, cuts)]
        local, acol, sums, pick = pl.pallas_call(
            functools.partial(anchor_kernel, starts=cuts[:-1]),
            compiler_params=LIMIT,
            in_specs=[whole(pltpu.SMEM), whole(pltpu.SMEM), whole(pltpu.HBM), whole(pltpu.HBM)],
            out_specs=[whole(), whole(), whole(), whole(pltpu.SMEM)],
            out_shape=[
                pltpu.VMEM(trip_counts.shape, trip_counts.dtype),
                pltpu.VMEM((bins, side, LANES), F32),
                pltpu.VMEM(((parts + 1) * slots, LANES), F32),
                jax.ShapeDtypeStruct((1,), jnp.int32),
            ],
            scratch_shapes=[pltpu.VMEM((bins, side), F32), pltpu.SemaphoreType.DMA((4 * bins + 1,))],
        )(place, block_columns, *far(anchor_hour, trip_counts))

        picked, span, *wanted = pl.pallas_call(
            functools.partial(lookup_kernel, ranges=ranges),
            compiler_params=LIMIT,
            in_specs=[whole(pltpu.SMEM), whole(pltpu.SMEM), whole(), whole()],
            out_specs=[whole()] * (2 + 2 * len(ranges)),
            out_shape=[
                pltpu.VMEM((parts, slots, LANES), F32),
                pltpu.VMEM((bins, width), F32),
            ]
            + [pltpu.VMEM((n, side // 4, side), F32) for _, n in ranges for _ in range(2)],
        )(place, block_columns, *near(dest_hour, daily_target))
        arrived, picked = gather(sums, n_orig, picked)

        quarter = side // 4
        gain, columns, opening, *sends = pl.pallas_call(
            functools.partial(day_kernel, ranges=ranges, count=len(arrived)),
            compiler_params=LIMIT,
            in_specs=[whole(pltpu.SMEM)] + [whole()] * (3 + len(arrived)),
            out_specs=[whole()] * (3 + 2 * len(ranges)),
            out_shape=[
                pltpu.VMEM((parts, slots, LANES), F32),
                pltpu.VMEM((n_orig, slots, LANES), F32),
                pltpu.VMEM((bins, ranges[0][1], side, side), trip_counts.dtype),
            ]
            + [pltpu.VMEM((n, quarter, side), F32) for _, n in ranges for _ in range(2)],
        )(place, *near(local, acol, picked, *arrived))

        def branch(k):
            def run(*args):
                return cycle(*args, ranges=ranges, used=k + 1)

            return run

        factors, final, fitted = lax.switch(
            pick[0],
            [branch(k) for k in range(len(ranges))],
            local,
            acol,
            gain,
            block_columns,
            place,
            wanted,
            sends,
        )
        block, final = pl.pallas_call(
            functools.partial(end_kernel, start=ranges[0][0]),
            compiler_params=LIMIT,
            in_specs=[whole(pltpu.SMEM)] + [whole()] * 8,
            out_specs=[whole(), whole()],
            out_shape=[
                pltpu.VMEM((bins, ranges[0][1], side, side), trip_counts.dtype),
                pltpu.VMEM((parts * slots, LANES), F32),
            ],
        )(place, *near(opening, acol, gain, *factors, final))
        fitted = pl.pallas_call(
            functools.partial(store_kernel, start=ranges[0][0]),
            compiler_params=LIMIT,
            in_specs=[whole(), whole(pltpu.HBM)],
            out_specs=whole(pltpu.HBM),
            out_shape=pltpu.HBM(trip_counts.shape, trip_counts.dtype),
            scratch_shapes=[pltpu.SemaphoreType.DMA((bins,))],
            input_output_aliases={1: 0},
        )(*near(block), *far(fitted))
        finals, fitted = gather(final, n_orig, fitted)
        gap = pl.pallas_call(
            gap_kernel,
            compiler_params=LIMIT,
            in_specs=[whole(pltpu.SMEM), whole(), whole()] + [whole()] * len(finals),
            out_specs=whole(),
            out_shape=jax.ShapeDtypeStruct((bins, width), F32),
        )(place, *near(span, columns, *finals))
        return fitted, gap

    return on_device


def solution(mesh):
    placed = (
        P("tm", "orig", None, None),
        P("tm", "orig"),
        P("tm", None),
        P("orig", None, None),
        P("orig"),
    )
    return jax.shard_map(
        make(mesh),
        mesh=mesh,
        in_specs=placed,
        out_specs=(P("tm", "orig", None, None), P("tm", "orig")),
        check_vma=False,
    )
```

```python
import functools

import jax
import jax.numpy as jnp
from jax import lax
from jax.experimental import pallas as pl
from jax.experimental.pallas import tpu as pltpu
from jax.sharding import PartitionSpec as P


LANES = 128
F32 = jnp.float32
LIMIT = pltpu.CompilerParams(vmem_limit_bytes=8 * 2**20)


def whole(memory_space=pltpu.VMEM):
    return pl.BlockSpec(memory_space=memory_space)


def near(*xs):
    return [pltpu.with_memory_space_constraint(x, pltpu.VMEM) for x in xs]


def far(*xs):
    return [pltpu.with_memory_space_constraint(x, pltpu.HBM) for x in xs]


def anchor_kernel(place, cols, anchor, trips, local, acol, sums, pick, margins, arrivals, *, starts):
    bins, slots, side, _ = trips.shape
    halves = side // LANES
    rows = side // 4
    first = pltpu.make_async_copy(anchor, margins, arrivals.at[4 * bins])
    first.start()
    blocks = [(t, r) for t in range(bins) for r in range(0, side, rows)]
    copies = [
        pltpu.make_async_copy(trips.at[t, :, r : r + rows, :], local.at[t, :, r : r + rows, :], arrivals.at[i])
        for i, (t, r) in enumerate(blocks)
    ]
    for copy in copies:
        copy.start()
    pick[0] = functools.reduce(lambda a, b: a + b, [(cols[s] >= 0).astype(jnp.int32) for s in starts])
    count = bins * halves * slots
    for s in range(slots):
        sums[count + s : count + s + 1, :] = jnp.full((1, LANES), cols[s], jnp.int32).astype(F32)
    live = [(cols[s] >= 0).astype(F32) for s in range(slots)]
    first.wait()
    for t, r in blocks:
        diagonal = (
            lax.broadcasted_iota(jnp.int32, (rows, side), 0) + r == lax.broadcasted_iota(jnp.int32, (rows, side), 1)
        )
        column = jnp.sum(jnp.where(diagonal, margins[t : t + 1, :], 0.0), axis=1, keepdims=True)
        acol[t, r : r + rows, :] = jnp.broadcast_to(column, (rows, LANES))

    def row_totals(t, r):
        total = None
        for s in range(slots):
            part = local[t, s, r : r + rows, :].astype(F32) * live[s]
            total = part if total is None else total + part
        return jnp.sum(total, axis=1, keepdims=True)

    def column_sums(t, r, total, acc):
        scale = acol[t, r : r + rows, :] / jnp.broadcast_to(total, (rows, LANES))
        acol[t, r : r + rows, :] = scale
        for s in range(slots):
            for h in range(halves):
                part = local[t, s, r : r + rows, h * LANES : (h + 1) * LANES].astype(F32) * scale
                part = jnp.sum(part.reshape(rows // 8, 8, LANES), axis=0)
                acc[s][h] = part if r == 0 else acc[s][h] + part
        if r + rows == side:
            for h in range(halves):
                for s in range(slots):
                    row = (t * halves + h) * slots + s
                    sums[row : row + 1, :] = jnp.sum(acc[s][h], axis=0, keepdims=True)

    acc = [[None] * halves for _ in range(slots)]
    waiting = None
    for copy, (t, r) in zip(copies, blocks):
        copy.wait()
        total = row_totals(t, r)
        if waiting is not None:
            column_sums(*waiting, acc)
        waiting = (t, r, total)
    column_sums(*waiting, acc)


def lookup_kernel(place, cols, dest, target, picked, span, *wanted, ranges):
    parts, slots, _ = picked.shape
    bins = dest.shape[0]
    halves = parts // bins
    side = halves * LANES
    for s in range(slots):
        start = pl.multiple_of(jnp.maximum(cols[s], 0) * side, side)
        row = dest[:, pl.ds(start, side)]
        for t in range(bins):
            for h in range(halves):
                picked[t * halves + h, s : s + 1, :] = row[t : t + 1, h * LANES : (h + 1) * LANES]
    width = span.shape[1]
    span[...] = dest[:, pl.ds(pl.multiple_of(place[1] * width, width), width)]
    for r, (start, count) in enumerate(ranges):
        for k, block in enumerate(blocks_of(place, True)):
            out = wanted[2 * r + k]
            out[...] = target[start : start + count, rows_of(block, out.shape[1]), :].astype(F32)


def matched(own, columns, values, parts, slots, first):
    acc = [jnp.zeros(own.shape, F32) for _ in range(parts)]
    at = 0
    for vref in values:
        for k in range(vref.shape[0]):
            cref, c = (vref, k) if columns is None else (columns, at)
            at += 1
            for s in range(slots):
                hit = own == cref[c, first + s : first + s + 1, :]
                for q in range(parts):
                    acc[q] = acc[q] + jnp.where(hit, vref[k, q * slots + s : q * slots + s + 1, :], 0.0)
    return acc


def gap_kernel(place, span, *refs):
    out = refs[-1]
    columns, values = refs[0], refs[1:-1]
    slots = columns.shape[1]
    first = values[0].shape[1]
    parts = first // slots
    bins = out.shape[0]
    halves = parts // bins
    side = halves * LANES
    blocks = out.shape[1] // side
    own = (lax.broadcasted_iota(jnp.int32, (blocks, LANES), 0) + place[1] * blocks).astype(F32)
    total = matched(own, columns, values, parts, slots, 0)
    for t in range(bins):
        for h in range(halves):
            for c in range(blocks):
                at = c * side + h * LANES
                out[t : t + 1, at : at + LANES] = total[t * halves + h][c : c + 1, :]
    out[...] = out[...] / span[...] - 1.0


def blocks_of(place, kept):
    first, second = place[0] >> 1, place[0] & 1
    if kept:
        return first, 2 + second
    return 1 - first, 3 - second


def rows_of(block, rows):
    return pl.ds(pl.multiple_of(block * rows, rows), rows)


def day_kernel(place, trips, acol, picked, *refs, ranges, count):
    arrived, gain, columns, outs = refs[:count], refs[count], refs[count + 1], refs[count + 2 :]
    bins, slots, side, _ = trips.shape
    halves = side // LANES
    parts = bins * halves
    first = parts * slots
    own = arrived[0][0, first : first + slots, :]
    total = matched(own, None, arrived, parts, slots, first)
    for q in range(parts):
        gain[q] = jnp.where(own >= 0.0, picked[q] / jnp.maximum(total[q], 1.0), 0.0)
    at = 0
    for ref in arrived:
        for k in range(ref.shape[0]):
            columns[at] = ref[k, first : first + slots, :]
            at += 1
    day_parts(place, trips, acol, gain, outs, ranges, False)


def keep_kernel(place, trips, acol, gain, *outs, ranges):
    day_parts(place, trips, acol, gain, outs, ranges, True)


def day_parts(place, trips, acol, gain, outs, ranges, kept):
    bins, _, side, _ = trips.shape
    halves = side // LANES
    rows = side // 4
    for k, block in enumerate(blocks_of(place, kept)):
        at = rows_of(block, rows)
        scale = [acol[t, at, :] for t in range(bins)]
        for r, (start, n) in enumerate(ranges):
            out = outs[2 * r + k]
            for i in range(n):
                for h in range(halves):
                    lanes = slice(h * LANES, (h + 1) * LANES)
                    acc = None
                    for t in range(bins):
                        q = t * halves + h
                        part = trips[t, start + i, at, lanes].astype(F32) * scale[t]
                        part = part * gain[q, start + i : start + i + 1, :]
                        acc = part if acc is None else acc + part
                    out[i, :, lanes] = acc


def fit_rows(place, trips, acol, gain, fa, fb, local, sums, start, kept):
    bins, _, side, _ = trips.shape
    slots = gain.shape[1]
    halves = side // LANES
    count, rows, _ = fa.shape
    places = [rows_of(block, rows) for block in blocks_of(place, kept)]
    scale = [[acol[t, at, :] for t in range(bins)] for at in places]
    for i in range(count):
        for t in range(bins):
            for h in range(halves):
                lanes = slice(h * LANES, (h + 1) * LANES)
                q = t * halves + h
                g = gain[q, start + i : start + i + 1, :]
                total = None
                for k, (at, factor) in enumerate(zip(places, (fa, fb))):
                    value = trips[t, start + i, at, lanes].astype(F32) * scale[k][t] * g * factor[i, :, lanes]
                    local[t, i, at, lanes] = value.astype(local.dtype)
                    part = jnp.sum(value.reshape(rows // 8, 8, LANES), axis=0)
                    total = part if total is None else total + part
                row = q * slots + start + i
                total = jnp.sum(total, axis=0, keepdims=True)
                sums[row : row + 1, :] = total if kept else sums[row : row + 1, :] + total


def copy_all(pairs, done):
    copies = [pltpu.make_async_copy(source, target, done.at[i]) for i, (source, target) in enumerate(pairs)]
    for copy in copies:
        copy.start()
    return copies


def copy_all(pairs, done, first=0):
    copies = [pltpu.make_async_copy(source, target, done.at[first + i]) for i, (source, target) in enumerate(pairs)]
    for copy in copies:
        copy.start()
    return copies


def empty_kernel(sums, fitted, blank, done, *, empty):
    sums[...] = jnp.zeros(sums.shape, F32)
    blank[...] = jnp.zeros(blank.shape, blank.dtype)
    for copy in copy_all([(blank, fitted.at[t, s]) for t in range(fitted.shape[0]) for s in empty], done):
        copy.wait()


def kept_kernel(place, trips, acol, gain, sums_in, *refs, ranges):
    n = len(ranges)
    factors, locals_, sums = refs[: 2 * n], refs[2 * n : 3 * n], refs[3 * n]
    sums[...] = sums_in[...]
    for r, (start, _) in enumerate(ranges):
        fit_rows(place, trips, acol, gain, factors[2 * r], factors[2 * r + 1], locals_[r], sums, start, True)


def rest_kernel(place, trips, acol, gain, fa, fb, sums_in, mine, local, sums, *refs, start):
    sums[...] = sums_in[...]
    fit_rows(place, trips, acol, gain, fa, fb, local, sums, start, False)
    if refs:
        fitted, done = refs
        bins, count, _, _ = local.shape
        for copy in copy_all([(local.at[t], fitted.at[t, start : start + count]) for t in range(bins)], done):
            copy.wait()


def end_kernel(place, trips, acol, gain, fa, fb, ga, gb, sums_in, *refs, start, ready_start, chained):
    refs = list(refs)
    copies = []
    if ready_start is None:
        local, sums = refs
    else:
        ready = refs.pop(0)
        if chained:
            refs.pop(0)
        local, sums, fitted, done = refs
        bins, count, _, _ = ready.shape
        copies = copy_all([(ready.at[t], fitted.at[t, ready_start : ready_start + count]) for t in range(bins)], done)
    sums[...] = sums_in[...]
    fit_rows(place, trips, acol, gain, fa, fb, local, sums, start, True)
    fit_rows(place, trips, acol, gain, ga, gb, local, sums, start, False)
    for copy in copies:
        copy.wait()


def store_kernel(local, before, fitted, done, *, start):
    bins, count, _, _ = local.shape
    for copy in copy_all([(local.at[t], fitted.at[t, start : start + count]) for t in range(bins)], done):
        copy.wait()


def cycle(trips, acol, gain, cols, place, wanted, sends, *, ranges):
    used = len(ranges)
    wanted = [wanted[2 * r + k][: ranges[r][1]] for r in range(used) for k in range(2)]
    sends = [sends[2 * r + k][: ranges[r][1]] for r in range(used) for k in range(2)]
    bins, slots, side, _ = trips.shape
    halves = side // LANES
    rows = side // 4
    parts = bins * halves
    order = range(used)[::-1]

    def over_first(x):
        return lax.ppermute(x, "tm", [(i, i ^ 2) for i in range(4)])

    def over_second(x):
        return lax.ppermute(x, "tm", [(i, i ^ 1) for i in range(4)])

    def factor(r, k, mine, other):
        start, count = ranges[r]
        empty = (cols[start : start + count] < 0).astype(F32)[:, None, None]
        return wanted[2 * r + k] / (mine + other + empty)

    def total(kept, got):
        return kept + got

    got = {r: (over_first(sends[2 * r]), over_second(sends[2 * r + 1])) for r in order}
    kept = pl.pallas_call(
        functools.partial(keep_kernel, ranges=ranges),
        compiler_params=LIMIT,
        in_specs=[whole(pltpu.SMEM)] + [whole()] * 3,
        out_specs=[whole()] * (2 * used),
        out_shape=[pltpu.VMEM((n, rows, side), F32) for _, n in ranges for _ in range(2)],
    )(place, *near(trips, acol, gain))
    mine = {r: [total(kept[2 * r + k], got[r][k]) for k in range(2)] for r in order}
    other = {r: (over_second(mine[r][0]), over_first(mine[r][1])) for r in order}
    scale = {r: [factor(r, k, mine[r][k], other[r][k]) for k in range(2)] for r in order}
    back = {r: (over_first(scale[r][0]), over_second(scale[r][1])) for r in order}
    shapes = [pltpu.VMEM((bins, n, side, side), trips.dtype) for _, n in ranges]
    final = pltpu.VMEM((parts * slots, LANES), F32)
    store = pltpu.HBM(trips.shape, trips.dtype)
    sums, fitted = jnp.zeros((parts * slots, LANES), F32), None
    empty = range(sum(count for _, count in ranges), slots)
    if empty:
        sums, fitted = pl.pallas_call(
            functools.partial(empty_kernel, empty=empty),
            compiler_params=LIMIT,
            out_specs=[whole(), whole(pltpu.HBM)],
            out_shape=[final, store],
            scratch_shapes=[pltpu.VMEM((side, side), trips.dtype), pltpu.SemaphoreType.DMA((bins * len(empty),))],
        )()
    if used > 1:
        *out, sums = pl.pallas_call(
            functools.partial(kept_kernel, ranges=ranges[1:]),
            compiler_params=LIMIT,
            in_specs=[whole(pltpu.SMEM)] + [whole()] * (4 + 2 * (used - 1)),
            out_specs=[whole()] * used,
            out_shape=[*shapes[1:used], final],
        )(place, *near(trips, acol, gain, sums, *[f for r in range(1, used) for f in scale[r]]))
        out = [None] + out
    else:
        out = [None]
    for r in order[:-1]:
        leaves = r > 1
        outs = pl.pallas_call(
            functools.partial(rest_kernel, start=ranges[r][0]),
            compiler_params=LIMIT,
            in_specs=[whole(pltpu.SMEM)] + [whole()] * 7,
            out_specs=[whole(), whole()] + [whole(pltpu.HBM)] * leaves,
            out_shape=[shapes[r], final] + [store] * leaves,
            scratch_shapes=[pltpu.SemaphoreType.DMA((bins,))] * leaves,
            input_output_aliases={7: 0},
        )(place, *near(trips, acol, gain, *back[r], sums, out[r]))
        out[r], sums = outs[:2]
        if leaves:
            fitted = outs[2]
    ready = [out[1]] if used > 1 else []
    outs = pl.pallas_call(
        functools.partial(
            end_kernel, start=ranges[0][0], ready_start=ranges[1][0] if ready else None, chained=len(ready) > 0
        ),
        compiler_params=LIMIT,
        in_specs=[whole(pltpu.SMEM)] + [whole()] * (8 + len(ready)) + [whole(pltpu.HBM)] * len(ready),
        out_specs=[whole(), whole()] + [whole(pltpu.HBM)] * len(ready),
        out_shape=[shapes[0], final] + [store] * len(ready),
        scratch_shapes=[pltpu.SemaphoreType.DMA((bins,))] * len(ready),
        input_output_aliases={10: 2} if ready else {},
    )(place, *near(trips, acol, gain, *scale[0], *back[0], sums, *ready), *(far(fitted) if ready else []))
    return outs[2] if ready else fitted, outs[0], outs[1]


def gather(x, n, beside):
    def swap(y, k):
        return lax.ppermute(y, "orig", [(i, i ^ k) for i in range(n)])

    distant = [swap(x, k) for k in range(n - 2, 0, -2)]
    distant, beside = lax.optimization_barrier((distant, beside))
    close = jnp.stack([x] + distant)
    return [close, swap(close, 1)], beside


def make(mesh):
    n_orig = mesh.shape["orig"]
    n_tm = mesh.shape["tm"]
    assert n_tm == 4 and n_orig & (n_orig - 1) == 0 and n_orig > 1

    def on_device(trip_counts, anchor_hour, dest_hour, daily_target, block_columns):
        bins, slots, side, _ = trip_counts.shape
        halves = side // LANES
        parts = bins * halves
        width = dest_hour.shape[1] // n_orig
        place = jnp.stack([lax.axis_index("tm").astype(jnp.int32), lax.axis_index("orig").astype(jnp.int32)])
        place, block_columns = lax.optimization_barrier((place, block_columns))

        ranges, plans = plans_of(slots)
        local, acol, sums, pick = pl.pallas_call(
            functools.partial(anchor_kernel, starts=[sum(n for _, n in plan) for plan in plans[:-1]]),
            compiler_params=LIMIT,
            in_specs=[whole(pltpu.SMEM), whole(pltpu.SMEM), whole(pltpu.HBM), whole(pltpu.HBM)],
            out_specs=[whole(), whole(), whole(), whole(pltpu.SMEM)],
            out_shape=[
                pltpu.VMEM(trip_counts.shape, trip_counts.dtype),
                pltpu.VMEM((bins, side, LANES), F32),
                pltpu.VMEM(((parts + 1) * slots, LANES), F32),
                jax.ShapeDtypeStruct((1,), jnp.int32),
            ],
            scratch_shapes=[pltpu.VMEM((bins, side), F32), pltpu.SemaphoreType.DMA((4 * bins + 1,))],
        )(place, block_columns, *far(anchor_hour, trip_counts))

        picked, span, *wanted = pl.pallas_call(
            functools.partial(lookup_kernel, ranges=ranges),
            compiler_params=LIMIT,
            in_specs=[whole(pltpu.SMEM), whole(pltpu.SMEM), whole(), whole()],
            out_specs=[whole()] * (2 + 2 * len(ranges)),
            out_shape=[
                pltpu.VMEM((parts, slots, LANES), F32),
                pltpu.VMEM((bins, width), F32),
            ]
            + [pltpu.VMEM((n, side // 4, side), F32) for _, n in ranges for _ in range(2)],
        )(place, block_columns, *near(dest_hour, daily_target))
        arrived, picked = gather(sums, n_orig, picked)

        quarter = side // 4
        gain, columns, *sends = pl.pallas_call(
            functools.partial(day_kernel, ranges=ranges, count=len(arrived)),
            compiler_params=LIMIT,
            in_specs=[whole(pltpu.SMEM)] + [whole()] * (3 + len(arrived)),
            out_specs=[whole()] * (2 + 2 * len(ranges)),
            out_shape=[
                pltpu.VMEM((parts, slots, LANES), F32),
                pltpu.VMEM((n_orig, slots, LANES), F32),
            ]
            + [pltpu.VMEM((n, quarter, side), F32) for _, n in ranges for _ in range(2)],
        )(place, *near(local, acol, picked, *arrived))

        def branch(k):
            def run(*args):
                return cycle(*args, ranges=plans[k])

            return run

        fitted, block, final = lax.switch(
            pick[0],
            [branch(k) for k in range(len(plans))],
            local,
            acol,
            gain,
            block_columns,
            place,
            wanted,
            sends,
        )
        fitted = pl.pallas_call(
            functools.partial(store_kernel, start=ranges[0][0]),
            compiler_params=LIMIT,
            in_specs=[whole(), whole(pltpu.HBM)],
            out_specs=whole(pltpu.HBM),
            out_shape=pltpu.HBM(trip_counts.shape, trip_counts.dtype),
            scratch_shapes=[pltpu.SemaphoreType.DMA((bins,))],
            input_output_aliases={1: 0},
        )(*near(block), *far(fitted))
        finals, fitted = gather(final, n_orig, fitted)
        gap = pl.pallas_call(
            gap_kernel,
            compiler_params=LIMIT,
            in_specs=[whole(pltpu.SMEM), whole(), whole()] + [whole()] * len(finals),
            out_specs=whole(),
            out_shape=jax.ShapeDtypeStruct((bins, width), F32),
        )(place, *near(span, columns, *finals))
        return fitted, gap

    return on_device


def plans_of(slots):
    small, half = max(slots // 6, 1), max(slots // 2, 2)
    ranges = [(0, small), (small, half - small), (half, slots - half)]
    plans = [ranges[:1]] + [[ranges[0], (small, n)] for n in range(1, half - small + 1)] + [ranges]
    return ranges, plans


def solution(mesh):
    placed = (
        P("tm", "orig", None, None),
        P("tm", "orig"),
        P("tm", None),
        P("orig", None, None),
        P("orig"),
    )
    step = jax.shard_map(
        make(mesh),
        mesh=mesh,
        in_specs=placed,
        out_specs=(P("tm", "orig", None, None), P("tm", "orig")),
        check_vma=False,
    )
    return lambda *args: step(*args)
```

```python
import functools

import jax
import jax.numpy as jnp
from jax import lax
from jax.experimental import pallas as pl
from jax.experimental.pallas import tpu as pltpu
from jax.sharding import PartitionSpec as P


LANES = 128
F32 = jnp.float32
LIMIT = pltpu.CompilerParams(vmem_limit_bytes=8 * 2**20)


def whole(memory_space=pltpu.VMEM):
    return pl.BlockSpec(memory_space=memory_space)


def near(*xs):
    return [pltpu.with_memory_space_constraint(x, pltpu.VMEM) for x in xs]


def far(*xs):
    return [pltpu.with_memory_space_constraint(x, pltpu.HBM) for x in xs]


def anchor_kernel(place, cols, anchor, trips, local, acol, sums, pick, margins, arrivals, *, starts):
    bins, slots, side, _ = trips.shape
    halves = side // LANES
    rows = side // 4
    first = pltpu.make_async_copy(anchor, margins, arrivals.at[4 * bins])
    first.start()
    blocks = [(t, r) for t in range(bins) for r in range(0, side, rows)]
    copies = [
        pltpu.make_async_copy(trips.at[t, :, r : r + rows, :], local.at[t, :, r : r + rows, :], arrivals.at[i])
        for i, (t, r) in enumerate(blocks)
    ]
    for copy in copies:
        copy.start()
    pick[0] = functools.reduce(lambda a, b: a + b, [(cols[s] >= 0).astype(jnp.int32) for s in starts])
    count = bins * halves * slots
    for s in range(slots):
        sums[count + s : count + s + 1, :] = jnp.full((1, LANES), cols[s], jnp.int32).astype(F32)
    live = [(cols[s] >= 0).astype(F32) for s in range(slots)]
    first.wait()
    for t, r in blocks:
        at = r // LANES * LANES
        diagonal = (
            lax.broadcasted_iota(jnp.int32, (rows, LANES), 0) + (r - at)
            == lax.broadcasted_iota(jnp.int32, (rows, LANES), 1)
        )
        column = jnp.sum(jnp.where(diagonal, margins[t : t + 1, at : at + LANES], 0.0), axis=1, keepdims=True)
        acol[t, r : r + rows, :] = jnp.broadcast_to(column, (rows, LANES))

    def row_totals(t, r):
        total = None
        for s in range(slots):
            part = (local[t, s, r : r + rows, :] * live[s].astype(local.dtype)).astype(F32)
            total = part if total is None else total + part
        return jnp.sum(total, axis=1, keepdims=True)

    def column_sums(t, r, total, acc):
        scale = acol[t, r : r + rows, :] / jnp.broadcast_to(total, (rows, LANES))
        acol[t, r : r + rows, :] = scale
        for s in range(slots):
            for h in range(halves):
                part = local[t, s, r : r + rows, h * LANES : (h + 1) * LANES].astype(F32) * scale
                part = jnp.sum(part.reshape(rows // 8, 8, LANES), axis=0)
                acc[s][h] = part if r == 0 else acc[s][h] + part
        if r + rows == side:
            for h in range(halves):
                for s in range(slots):
                    row = (t * halves + h) * slots + s
                    sums[row : row + 1, :] = jnp.sum(acc[s][h], axis=0, keepdims=True)

    acc = [[None] * halves for _ in range(slots)]
    waiting = None
    for copy, (t, r) in zip(copies, blocks):
        copy.wait()
        total = row_totals(t, r)
        if waiting is not None:
            column_sums(*waiting, acc)
        waiting = (t, r, total)
    column_sums(*waiting, acc)


def lookup_kernel(place, cols, dest, target, picked, span, *wanted, ranges):
    parts, slots, _ = picked.shape
    bins = dest.shape[0]
    halves = parts // bins
    side = halves * LANES
    for s in range(slots):
        start = pl.multiple_of(jnp.maximum(cols[s], 0) * side, side)
        row = dest[:, pl.ds(start, side)]
        for t in range(bins):
            for h in range(halves):
                picked[t * halves + h, s : s + 1, :] = row[t : t + 1, h * LANES : (h + 1) * LANES]
    width = span.shape[1]
    span[...] = dest[:, pl.ds(pl.multiple_of(place[1] * width, width), width)]
    for r, (start, count) in enumerate(ranges):
        for k, block in enumerate(blocks_of(place, True)):
            out = wanted[2 * r + k]
            out[...] = target[start : start + count, rows_of(block, out.shape[1]), :].astype(F32)


def matched(own, columns, values, parts, slots, first):
    acc = [jnp.zeros(own.shape, F32) for _ in range(parts)]
    at = 0
    for vref in values:
        for k in range(vref.shape[0]):
            cref, c = (vref, k) if columns is None else (columns, at)
            at += 1
            for s in range(slots):
                hit = own == cref[c, first + s : first + s + 1, :]
                for q in range(parts):
                    acc[q] = acc[q] + jnp.where(hit, vref[k, q * slots + s : q * slots + s + 1, :], 0.0)
    return acc


def gap_kernel(place, span, *refs):
    out = refs[-1]
    columns, values = refs[0], refs[1:-1]
    slots = columns.shape[1]
    first = values[0].shape[1]
    parts = first // slots
    bins = out.shape[0]
    halves = parts // bins
    side = halves * LANES
    blocks = out.shape[1] // side
    own = (lax.broadcasted_iota(jnp.int32, (blocks, LANES), 0) + place[1] * blocks).astype(F32)
    total = matched(own, columns, values, parts, slots, 0)
    for t in range(bins):
        for h in range(halves):
            for c in range(blocks):
                at = c * side + h * LANES
                out[t : t + 1, at : at + LANES] = total[t * halves + h][c : c + 1, :]
    out[...] = out[...] / span[...] - 1.0


def blocks_of(place, kept):
    first, second = place[0] >> 1, place[0] & 1
    if kept:
        return first, 2 + second
    return 1 - first, 3 - second


def rows_of(block, rows):
    return pl.ds(pl.multiple_of(block * rows, rows), rows)


def day_kernel(place, trips, acol, picked, *refs, ranges, count):
    arrived, gain, columns, outs = refs[:count], refs[count], refs[count + 1], refs[count + 2 :]
    bins, slots, side, _ = trips.shape
    halves = side // LANES
    parts = bins * halves
    first = parts * slots
    own = arrived[0][0, first : first + slots, :]
    total = matched(own, None, arrived, parts, slots, first)
    for q in range(parts):
        gain[q] = jnp.where(own >= 0.0, picked[q] / jnp.maximum(total[q], 1.0), 0.0)
    at = 0
    for ref in arrived:
        for k in range(ref.shape[0]):
            columns[at] = ref[k, first : first + slots, :]
            at += 1
    day_parts(place, trips, acol, gain, outs, ranges, False)


def keep_kernel(place, trips, acol, gain, *outs, ranges):
    day_parts(place, trips, acol, gain, outs, ranges, True)


def day_parts(place, trips, acol, gain, outs, ranges, kept):
    bins, _, side, _ = trips.shape
    halves = side // LANES
    rows = side // 4
    for k, block in enumerate(blocks_of(place, kept)):
        at = rows_of(block, rows)
        scale = [acol[t, at, :] for t in range(bins)]
        for r, (start, n) in enumerate(ranges):
            out = outs[2 * r + k]
            for i in range(n):
                for h in range(halves):
                    lanes = slice(h * LANES, (h + 1) * LANES)
                    acc = None
                    for t in range(bins):
                        q = t * halves + h
                        part = trips[t, start + i, at, lanes].astype(F32) * scale[t]
                        part = part * gain[q, start + i : start + i + 1, :]
                        acc = part if acc is None else acc + part
                    out[i, :, lanes] = acc


def fit_rows(place, trips, acol, gain, fa, fb, local, sums, start, kept):
    bins, _, side, _ = trips.shape
    slots = gain.shape[1]
    halves = side // LANES
    count, rows, _ = fa.shape
    places = [rows_of(block, rows) for block in blocks_of(place, kept)]
    scale = [[acol[t, at, :] for t in range(bins)] for at in places]
    for i in range(count):
        for t in range(bins):
            for h in range(halves):
                lanes = slice(h * LANES, (h + 1) * LANES)
                q = t * halves + h
                g = gain[q, start + i : start + i + 1, :]
                total = None
                for k, (at, factor) in enumerate(zip(places, (fa, fb))):
                    value = trips[t, start + i, at, lanes].astype(F32) * scale[k][t] * g * factor[i, :, lanes]
                    local[t, i, at, lanes] = value.astype(local.dtype)
                    part = jnp.sum(value.reshape(rows // 8, 8, LANES), axis=0)
                    total = part if total is None else total + part
                row = q * slots + start + i
                total = jnp.sum(total, axis=0, keepdims=True)
                sums[row : row + 1, :] = total if kept else sums[row : row + 1, :] + total


def copy_all(pairs, done):
    copies = [pltpu.make_async_copy(source, target, done.at[i]) for i, (source, target) in enumerate(pairs)]
    for copy in copies:
        copy.start()
    return copies


def copy_all(pairs, done, first=0):
    copies = [pltpu.make_async_copy(source, target, done.at[first + i]) for i, (source, target) in enumerate(pairs)]
    for copy in copies:
        copy.start()
    return copies


def empty_kernel(sums, fitted, blank, done, *, empty):
    sums[...] = jnp.zeros(sums.shape, F32)
    blank[...] = jnp.zeros(blank.shape, blank.dtype)
    for copy in copy_all([(blank, fitted.at[t, s]) for t in range(fitted.shape[0]) for s in empty], done):
        copy.wait()


def kept_kernel(place, trips, acol, gain, sums_in, *refs, ranges):
    n = len(ranges)
    factors, locals_, sums = refs[: 2 * n], refs[2 * n : 3 * n], refs[3 * n]
    sums[...] = sums_in[...]
    for r, (start, _) in enumerate(ranges):
        fit_rows(place, trips, acol, gain, factors[2 * r], factors[2 * r + 1], locals_[r], sums, start, True)


def rest_kernel(place, trips, acol, gain, fa, fb, sums_in, mine, local, sums, *refs, start):
    sums[...] = sums_in[...]
    fit_rows(place, trips, acol, gain, fa, fb, local, sums, start, False)
    if refs:
        fitted, done = refs
        bins, count, _, _ = local.shape
        for copy in copy_all([(local.at[t], fitted.at[t, start : start + count]) for t in range(bins)], done):
            copy.wait()


def end_kernel(place, trips, acol, gain, fa, fb, ga, gb, sums_in, *refs, start, ready_start, chained):
    refs = list(refs)
    copies = []
    if ready_start is None:
        local, sums = refs
    else:
        ready = refs.pop(0)
        if chained:
            refs.pop(0)
        local, sums, fitted, done = refs
        bins, count, _, _ = ready.shape
        copies = copy_all([(ready.at[t], fitted.at[t, ready_start : ready_start + count]) for t in range(bins)], done)
    sums[...] = sums_in[...]
    fit_rows(place, trips, acol, gain, fa, fb, local, sums, start, True)
    fit_rows(place, trips, acol, gain, ga, gb, local, sums, start, False)
    for copy in copies:
        copy.wait()


def store_kernel(local, before, fitted, done, *, start):
    bins, count, _, _ = local.shape
    for copy in copy_all([(local.at[t], fitted.at[t, start : start + count]) for t in range(bins)], done):
        copy.wait()


def cycle(trips, acol, gain, cols, place, wanted, sends, *, ranges):
    used = len(ranges)
    wanted = [wanted[2 * r + k][: ranges[r][1]] for r in range(used) for k in range(2)]
    sends = [sends[2 * r + k][: ranges[r][1]] for r in range(used) for k in range(2)]
    bins, slots, side, _ = trips.shape
    halves = side // LANES
    rows = side // 4
    parts = bins * halves
    order = range(used)[::-1]

    def over_first(x):
        return lax.ppermute(x, "tm", [(i, i ^ 2) for i in range(4)])

    def over_second(x):
        return lax.ppermute(x, "tm", [(i, i ^ 1) for i in range(4)])

    def factor(r, k, mine, other):
        start, count = ranges[r]
        empty = (cols[start : start + count] < 0).astype(F32)[:, None, None]
        return wanted[2 * r + k] / (mine + other + empty)

    def total(kept, got):
        return kept + got

    got = {r: (over_first(sends[2 * r]), over_second(sends[2 * r + 1])) for r in order}
    kept = pl.pallas_call(
        functools.partial(keep_kernel, ranges=ranges),
        compiler_params=LIMIT,
        in_specs=[whole(pltpu.SMEM)] + [whole()] * 3,
        out_specs=[whole()] * (2 * used),
        out_shape=[pltpu.VMEM((n, rows, side), F32) for _, n in ranges for _ in range(2)],
    )(place, *near(trips, acol, gain))
    mine = {r: [total(kept[2 * r + k], got[r][k]) for k in range(2)] for r in order}
    other = {r: (over_second(mine[r][0]), over_first(mine[r][1])) for r in order}
    scale = {r: [factor(r, k, mine[r][k], other[r][k]) for k in range(2)] for r in order}
    back = {r: (over_first(scale[r][0]), over_second(scale[r][1])) for r in order}
    shapes = [pltpu.VMEM((bins, n, side, side), trips.dtype) for _, n in ranges]
    final = pltpu.VMEM((parts * slots, LANES), F32)
    store = pltpu.HBM(trips.shape, trips.dtype)
    sums, fitted = jnp.zeros((parts * slots, LANES), F32), None
    empty = range(sum(count for _, count in ranges), slots)
    if empty:
        sums, fitted = pl.pallas_call(
            functools.partial(empty_kernel, empty=empty),
            compiler_params=LIMIT,
            out_specs=[whole(), whole(pltpu.HBM)],
            out_shape=[final, store],
            scratch_shapes=[pltpu.VMEM((side, side), trips.dtype), pltpu.SemaphoreType.DMA((bins * len(empty),))],
        )()
    if used > 1:
        *out, sums = pl.pallas_call(
            functools.partial(kept_kernel, ranges=ranges[1:]),
            compiler_params=LIMIT,
            in_specs=[whole(pltpu.SMEM)] + [whole()] * (4 + 2 * (used - 1)),
            out_specs=[whole()] * used,
            out_shape=[*shapes[1:used], final],
        )(place, *near(trips, acol, gain, sums, *[f for r in range(1, used) for f in scale[r]]))
        out = [None] + out
    else:
        out = [None]
    for r in order[:-1]:
        leaves = r > 1
        outs = pl.pallas_call(
            functools.partial(rest_kernel, start=ranges[r][0]),
            compiler_params=LIMIT,
            in_specs=[whole(pltpu.SMEM)] + [whole()] * 7,
            out_specs=[whole(), whole()] + [whole(pltpu.HBM)] * leaves,
            out_shape=[shapes[r], final] + [store] * leaves,
            scratch_shapes=[pltpu.SemaphoreType.DMA((bins,))] * leaves,
            input_output_aliases={7: 0},
        )(place, *near(trips, acol, gain, *back[r], sums, out[r]))
        out[r], sums = outs[:2]
        if leaves:
            fitted = outs[2]
    ready = [out[1]] if used > 1 else []
    outs = pl.pallas_call(
        functools.partial(
            end_kernel, start=ranges[0][0], ready_start=ranges[1][0] if ready else None, chained=len(ready) > 0
        ),
        compiler_params=LIMIT,
        in_specs=[whole(pltpu.SMEM)] + [whole()] * (8 + len(ready)) + [whole(pltpu.HBM)] * len(ready),
        out_specs=[whole(), whole()] + [whole(pltpu.HBM)] * len(ready),
        out_shape=[shapes[0], final] + [store] * len(ready),
        scratch_shapes=[pltpu.SemaphoreType.DMA((bins,))] * len(ready),
        input_output_aliases={10: 2} if ready else {},
    )(place, *near(trips, acol, gain, *scale[0], *back[0], sums, *ready), *(far(fitted) if ready else []))
    return outs[2] if ready else fitted, outs[0], outs[1]


def gather(x, n, beside):
    def swap(y, k):
        return lax.ppermute(y, "orig", [(i, i ^ k) for i in range(n)])

    distant = [swap(x, k) for k in range(n - 2, 0, -2)]
    distant, beside = lax.optimization_barrier((distant, beside))
    close = jnp.stack([x] + distant)
    return [close, swap(close, 1)], beside


def make(mesh):
    n_orig = mesh.shape["orig"]
    n_tm = mesh.shape["tm"]
    assert n_tm == 4 and n_orig & (n_orig - 1) == 0 and n_orig > 1

    def on_device(trip_counts, anchor_hour, dest_hour, daily_target, block_columns):
        bins, slots, side, _ = trip_counts.shape
        halves = side // LANES
        parts = bins * halves
        width = dest_hour.shape[1] // n_orig
        place = jnp.stack([lax.axis_index("tm").astype(jnp.int32), lax.axis_index("orig").astype(jnp.int32)])
        place, block_columns = lax.optimization_barrier((place, block_columns))

        ranges, plans = plans_of(slots)
        local, acol, sums, pick = pl.pallas_call(
            functools.partial(anchor_kernel, starts=[sum(n for _, n in plan) for plan in plans[:-1]]),
            compiler_params=LIMIT,
            in_specs=[whole(pltpu.SMEM), whole(pltpu.SMEM), whole(pltpu.HBM), whole(pltpu.HBM)],
            out_specs=[whole(), whole(), whole(), whole(pltpu.SMEM)],
            out_shape=[
                pltpu.VMEM(trip_counts.shape, trip_counts.dtype),
                pltpu.VMEM((bins, side, LANES), F32),
                pltpu.VMEM(((parts + 1) * slots, LANES), F32),
                jax.ShapeDtypeStruct((1,), jnp.int32),
            ],
            scratch_shapes=[pltpu.VMEM((bins, side), F32), pltpu.SemaphoreType.DMA((4 * bins + 1,))],
        )(place, block_columns, *far(anchor_hour, trip_counts))

        picked, span, *wanted = pl.pallas_call(
            functools.partial(lookup_kernel, ranges=ranges),
            compiler_params=LIMIT,
            in_specs=[whole(pltpu.SMEM), whole(pltpu.SMEM), whole(), whole()],
            out_specs=[whole()] * (2 + 2 * len(ranges)),
            out_shape=[
                pltpu.VMEM((parts, slots, LANES), F32),
                pltpu.VMEM((bins, width), F32),
            ]
            + [pltpu.VMEM((n, side // 4, side), F32) for _, n in ranges for _ in range(2)],
        )(place, block_columns, *near(dest_hour, daily_target))
        arrived, picked = gather(sums, n_orig, picked)

        quarter = side // 4
        gain, columns, *sends = pl.pallas_call(
            functools.partial(day_kernel, ranges=ranges, count=len(arrived)),
            compiler_params=LIMIT,
            in_specs=[whole(pltpu.SMEM)] + [whole()] * (3 + len(arrived)),
            out_specs=[whole()] * (2 + 2 * len(ranges)),
            out_shape=[
                pltpu.VMEM((parts, slots, LANES), F32),
                pltpu.VMEM((n_orig, slots, LANES), F32),
            ]
            + [pltpu.VMEM((n, quarter, side), F32) for _, n in ranges for _ in range(2)],
        )(place, *near(local, acol, picked, *arrived))

        def branch(k):
            def run(*args):
                return cycle(*args, ranges=plans[k])

            return run

        fitted, block, final = lax.switch(
            pick[0],
            [branch(k) for k in range(len(plans))],
            local,
            acol,
            gain,
            block_columns,
            place,
            wanted,
            sends,
        )
        fitted = pl.pallas_call(
            functools.partial(store_kernel, start=ranges[0][0]),
            compiler_params=LIMIT,
            in_specs=[whole(), whole(pltpu.HBM)],
            out_specs=whole(pltpu.HBM),
            out_shape=pltpu.HBM(trip_counts.shape, trip_counts.dtype),
            scratch_shapes=[pltpu.SemaphoreType.DMA((bins,))],
            input_output_aliases={1: 0},
        )(*near(block), *far(fitted))
        finals, fitted = gather(final, n_orig, fitted)
        gap = pl.pallas_call(
            gap_kernel,
            compiler_params=LIMIT,
            in_specs=[whole(pltpu.SMEM), whole(), whole()] + [whole()] * len(finals),
            out_specs=whole(),
            out_shape=jax.ShapeDtypeStruct((bins, width), F32),
        )(place, *near(span, columns, *finals))
        return fitted, gap

    return on_device


def plans_of(slots):
    small, half = max(slots // 6, 1), max(slots // 2, 2)
    ranges = [(0, small), (small, half - small), (half, slots - half)]
    plans = [ranges[:1]] + [[ranges[0], (small, n)] for n in range(1, half - small + 1)] + [ranges]
    return ranges, plans


def solution(mesh):
    placed = (
        P("tm", "orig", None, None),
        P("tm", "orig"),
        P("tm", None),
        P("orig", None, None),
        P("orig"),
    )
    step = jax.shard_map(
        make(mesh),
        mesh=mesh,
        in_specs=placed,
        out_specs=(P("tm", "orig", None, None), P("tm", "orig")),
        check_vma=False,
    )
    return lambda *args: step(*args)
```
